256 devices in a mesh: dom: 64 (over z, y, core), sub: 4 (over x).
Axes of the slice: x: 4, y: 4, z: 8, core: 2. Of those that a mesh axis runs over, the one named last changes fastest.
Arguments:
- diag_block: bfloat16 [30, 30, 32768], P(None, None, ('dom', 'sub')), may hold values from -6 to 6
- face_block: bfloat16 [6, 30, 30, 32768], P(None, None, None, ('dom', 'sub')), may hold values from -3 to 3
- restrict1: bfloat16 [30, 30, 32768], P(None, None, ('dom', 'sub')), may hold values from -1 to 1
- neighbour: int32 [6, 32768], P(None, ('dom', 'sub')), may hold values from 0 to 319
- face_slot: int32 [6, 32768], P(None, ('dom', 'sub')), may hold values from 0 to 7
- agg_map: int32 [32768], P(('dom', 'sub')), may hold values from 0 to 15, as said below
- send_list: int32 [6, 8192], P(None, ('dom', 'sub')), may hold values from 0 to 127
- restrict2: float32 [30, 30, 4096], P(None, None, ('dom', 'sub')), may hold values from -0.5 to 0.5
- coarse_nbr: int32 [8, 4096], P(None, ('dom', 'sub')), may hold values from 0 to 63
- agg2_map: int32 [4096], P(('dom', 'sub')), may hold values from 0 to 7, as said below
- coarse_slot: int32 [8, 4096], P(None, ('dom', 'sub')), may hold values from 0 to 7
Outputs:
- coarse_one: float32 [8, 30, 30, 4096], P(None, None, None, ('dom', 'sub'))
- coarse_two: float32 [8, 30, 30, 512], P(None, None, None, ('dom', 'sub'))
The draws below stay inside these ranges and needn't reach their ends.
Inputs may be any that keep to these rules, and one draw needn't show every extreme that they name: `neighbour`: positions below 128 name the device's own elements; position 128 + r * 32 + h names entry h of the list that the partition at offset o_r sends. `agg_map`: on each device every value is taken by exactly 8 elements. `send_list`: indices of the device's own elements. `coarse_nbr`: index among the subgroup's first-level agglomerates, in device order. `agg2_map`: within each subgroup every value is taken by exactly 8 first-level agglomerates.
All inputs are finite; a program needn't handle non-finite values.
Results may differ from the reference program's by a relative error of at most 0.0029.
Values may be sent and summed in bfloat16 or wider, within the bound.
A program may use at most 128 MiB of HBM per device.

```python
import jax
import jax.numpy as jnp
from jax import lax

NB = 30
E_DEV = 128
FACES = 6
SLOTS1 = 8
SLOTS2 = 8
RANGE = 3
HALO = 32
ELEMS = 32768
AGGS1 = 4096
N_DOM = 64
N_SUB = 4
DEVICES = 256


def draw_agg_map(key, part):
    keys = jax.random.split(jax.random.fold_in(key, 11), N_DOM * N_SUB)
    shuffled = jax.vmap(lambda single_key: jax.random.permutation(single_key, E_DEV))(keys)
    return (shuffled // 8).reshape(-1).astype(jnp.int32)


def draw_agg2_map(key, part):
    keys = jax.random.split(jax.random.fold_in(key, 23), N_DOM)
    shuffled = jax.vmap(lambda single_key: jax.random.permutation(single_key, N_SUB * (E_DEV // 8)))(keys)
    return (shuffled // 8).reshape(-1).astype(jnp.int32)


def set_ends(array, own_key, least, high):
    shape = array.shape
    place = [jax.random.randint(jax.random.fold_in(own_key, axis), (), 0, shape[axis]) for axis in range(len(shape))]
    array = array.at[tuple(place)].set(least)
    longest = shape.index(max(shape))
    place[longest] = (place[longest] + 1) % shape[longest]
    return array.at[tuple(place)].set(high)


def block_scale(own_key, extent, cuts, smallest, top_value):
    level = 1.0
    for dim, parts in cuts:
        heights = jax.random.uniform(jax.random.fold_in(jax.random.fold_in(own_key, 6), dim), (parts,), jnp.float32, smallest / len(cuts), top_value / len(cuts))
        level = level * jnp.repeat(jnp.exp(heights), extent[dim] // parts).reshape((-1,) + (1,) * (len(extent) - 1 - dim))
    return level


def centred(stream_key, dims, width, reach, shards=(), held_as=jnp.bfloat16):
    drawn = width * jax.random.normal(stream_key, dims, jnp.float32)
    if shards:
        drawn = drawn * block_scale(stream_key, dims, shards, -0.22, 0.18)
    return jnp.clip(drawn, -reach, reach).astype(held_as)


def setup_inputs(seed: int = 0) -> dict:
    splits = jax.random.split(jax.random.key(seed), 12)
    return {
        "diag_block": centred(splits[0], (NB, NB, ELEMS), 1.0, 6.0, ((2, 256),)),
        "face_block": centred(splits[1], (FACES, NB, NB, ELEMS), 0.5, 3.0, ((3, 256),)),
        "restrict1": centred(splits[2], (NB, NB, ELEMS), NB ** -0.5, 1.0, ((2, 256),)),
        "neighbour": set_ends(jax.random.randint(splits[3], (FACES, ELEMS), 0, E_DEV + 2 * RANGE * HALO), jax.random.fold_in(splits[3], 1), 0, (E_DEV + 2 * RANGE * HALO) - 1).astype(jnp.int32),
        "face_slot": set_ends(jax.random.randint(splits[4], (FACES, ELEMS), 0, SLOTS1), jax.random.fold_in(splits[4], 1), 0, SLOTS1 - 1).astype(jnp.int32),
        "agg_map": draw_agg_map(jax.random.fold_in(splits[11], 71), 0),
        "send_list": set_ends(jax.random.randint(splits[6], (2 * RANGE, DEVICES * HALO), 0, E_DEV), jax.random.fold_in(splits[6], 1), 0, E_DEV - 1).astype(jnp.int32),
        "restrict2": centred(splits[7], (NB, NB, AGGS1), (4 * NB) ** -0.5, 0.5, ((2, 256),), jnp.float32),
        "coarse_nbr": set_ends(jax.random.randint(splits[8], (SLOTS1, AGGS1), 0, N_SUB * (E_DEV // 8)), jax.random.fold_in(splits[8], 1), 0, (N_SUB * (E_DEV // 8)) - 1).astype(jnp.int32),
        "agg2_map": draw_agg2_map(jax.random.fold_in(splits[11], 71), 0),
        "coarse_slot": set_ends(jax.random.randint(splits[10], (SLOTS1, AGGS1), 0, SLOTS2), jax.random.fold_in(splits[10], 1), 0, SLOTS2 - 1).astype(jnp.int32),
    }


exact = lax.Precision.HIGHEST


def round_half(values):
    return lax.optimization_barrier(values.astype(jnp.bfloat16)).astype(jnp.float32)


def peer_offsets():
    return [step_index - RANGE if step_index < RANGE else step_index - RANGE + 1 for step_index in range(2 * RANGE)]


def level_one(device, diag_block, face_block, restrict1, neighbour, face_slot, agg_map, send_list):
    dom_index = device // N_SUB
    sub_index = device % N_SUB
    first_row = device * E_DEV
    own_maps = lax.dynamic_slice_in_dim(restrict1, first_row, E_DEV, 2)
    pieces = [own_maps]
    for step_index, offset in enumerate(peer_offsets()):
        source = ((dom_index + offset) % N_DOM) * N_SUB + sub_index
        listed = lax.dynamic_slice_in_dim(send_list[step_index], source * HALO, HALO, 0)
        pieces.append(jnp.take(restrict1, (source * E_DEV + listed).astype(jnp.int32), axis=2))
    extended = jnp.concatenate(pieces, axis=2).astype(jnp.float32)
    own_float = own_maps.astype(jnp.float32)
    diag_here = lax.dynamic_slice_in_dim(diag_block, first_row, E_DEV, 2).astype(jnp.float32)
    faces_here = lax.dynamic_slice_in_dim(face_block, first_row, E_DEV, 3).astype(jnp.float32)
    link_ids = lax.dynamic_slice_in_dim(neighbour, first_row, E_DEV, 1)
    slot_ids = lax.dynamic_slice_in_dim(face_slot, first_row, E_DEV, 1)
    groups = lax.dynamic_slice_in_dim(agg_map, first_row, E_DEV, 0)
    own_half = round_half(jnp.einsum('imb,jmb->ijb', diag_here, own_float, precision=exact))
    self_term = jnp.einsum('aib,ijb->ajb', own_float, own_half, precision=exact)
    far_maps = jnp.take(extended, link_ids.reshape(-1), axis=2).reshape(NB, NB, FACES, E_DEV)
    face_half = round_half(jnp.einsum('kimb,jmkb->kijb', faces_here, far_maps, precision=exact))
    face_term = jnp.einsum('aib,kijb->kajb', own_float, face_half, precision=exact)
    slot_index = jnp.arange(SLOTS1, dtype=jnp.int32)
    slot_pick = (slot_ids[None] == slot_index[:, None, None]).astype(jnp.float32)
    first_slot = (slot_index == 0).astype(jnp.float32)[:, None, None, None]
    per_elem = jnp.einsum('skb,kajb->sajb', slot_pick, face_term, precision=exact) + first_slot * self_term[None]
    summed = jax.ops.segment_sum(jnp.moveaxis(per_elem, 3, 0), groups, num_segments=E_DEV // 8)
    return jnp.moveaxis(summed, 0, 3)


def level_two(group, coarse_one, restrict2, coarse_nbr, agg2_map, coarse_slot):
    member_count = N_SUB * (E_DEV // 8)
    owned_count = member_count // 8
    first_row = group * member_count
    blocks = lax.dynamic_slice_in_dim(coarse_one, first_row, member_count, 3)
    level_maps = lax.dynamic_slice_in_dim(restrict2, first_row, member_count, 2)
    link_ids = lax.dynamic_slice_in_dim(coarse_nbr, first_row, member_count, 1)
    groups = lax.dynamic_slice_in_dim(agg2_map, first_row, member_count, 0)
    slot_ids = lax.dynamic_slice_in_dim(coarse_slot, first_row, member_count, 1)
    far_maps = jnp.take(level_maps, link_ids.reshape(-1), axis=2).reshape(NB, NB, SLOTS1, member_count)
    right_half = jnp.einsum('sijb,kjsb->sikb', blocks, far_maps, precision=exact)
    products = jnp.einsum('aib,sikb->sakb', level_maps, right_half, precision=exact)
    targets = (slot_ids * owned_count + groups[None]).reshape(-1).astype(jnp.int32)
    item_rows = jnp.moveaxis(products, 3, 1).reshape(SLOTS1 * member_count, NB, NB)
    summed = jax.ops.segment_sum(item_rows, targets, num_segments=SLOTS2 * owned_count)
    return jnp.moveaxis(summed.reshape(SLOTS2, owned_count, NB, NB), 1, 3)


def reference(diag_block, face_block, restrict1, neighbour, face_slot, agg_map, send_list, restrict2, coarse_nbr, agg2_map, coarse_slot):
    devices = jnp.arange(N_DOM * N_SUB, dtype=jnp.int32)
    per_device = lax.map(lambda device: level_one(device, diag_block, face_block, restrict1, neighbour, face_slot, agg_map, send_list), devices)
    coarse_one = jnp.moveaxis(per_device, 0, 3).reshape(SLOTS1, NB, NB, -1)
    subgroups = jnp.arange(N_DOM, dtype=jnp.int32)
    per_group = lax.map(lambda group: level_two(group, coarse_one, restrict2, coarse_nbr, agg2_map, coarse_slot), subgroups)
    coarse_two = jnp.moveaxis(per_group, 0, 3).reshape(SLOTS2, NB, NB, -1)
    return (coarse_one, coarse_two)
```

```python
import functools

import jax
import jax.numpy as jnp
from jax import lax
from jax.experimental import pallas as pl
from jax.experimental.pallas import tpu as pltpu
from jax.sharding import PartitionSpec as P

NB = 30
PAD = 32
PITCH = 40
LANES = 128
FACES = 6
SLOTS = 8
HALO = 32
REACH = 3
PEERS = 6
GROUPS = 4
ROWS = NB * PAD
QUARTER = ROWS // GROUPS
AGGS = 16
SUBS = 4
F32 = jnp.float32
BF16 = jnp.bfloat16
MESH = pl.DeviceIdType.MESH
OFFSETS = tuple(r - REACH if r < REACH else r - REACH + 1 for r in range(PEERS))


def iota(shape, dim):
    return lax.broadcasted_iota(jnp.int32, shape, dim)


def dot(a, b):
    return jnp.dot(a, b, preferred_element_type=F32)


def split(x):
    high = x.astype(BF16)
    return high, (x - high.astype(F32)).astype(BF16)


def turn_maps(restrict_ref, wide_ref, turned_ref):
    wide_ref[pl.ds(NB * PITCH, 2 * PITCH), :] = jnp.zeros((2 * PITCH, LANES), F32)
    for n in range(NB):
        wide_ref[pl.ds(n * PITCH, NB), :] = restrict_ref[n].astype(F32)
    for m in range(NB):
        turned_ref[pl.ds(m * PAD, PAD), :] = wide_ref[pl.ds(m, PAD, stride=PITCH), :].astype(BF16)


def pack_messages(turned_ref, list_ref, message_ref):
    lane_group = iota((QUARTER, LANES), 1) // HALO
    rows = turned_ref[...]
    for r in range(PEERS):
        row = list_ref[pl.ds(r, 1), :]
        four = jnp.concatenate([row] * GROUPS, axis=1)
        pick = (iota((LANES, LANES), 0) == four).astype(BF16)
        chosen = dot(rows, pick)
        packed = jnp.zeros((QUARTER, LANES), F32)
        for q in range(GROUPS):
            packed = jnp.where(lane_group == q, chosen[q * QUARTER : (q + 1) * QUARTER], packed)
        message_ref[r] = packed.astype(BF16)


def send_kernel(
    restrict_ref, list_ref, coarse_ref, turned_ref, halo_ref, maps_ref,
    wide_ref, message_ref, landed_ref, gathered_ref, send_sem, recv_sem, map_send, map_recv,
):
    dom, sub = lax.axis_index("dom"), lax.axis_index("sub")
    doms, subs = lax.axis_size("dom"), lax.axis_size("sub")
    barrier = pltpu.get_barrier_semaphore()
    for offset in OFFSETS:
        peer = lax.rem(dom + offset + doms, doms)
        pl.semaphore_signal(barrier, inc=1, device_id=(peer, sub), device_id_type=MESH)
    for step in range(1, SUBS):
        peer = lax.rem(sub + step, subs)
        pl.semaphore_signal(barrier, inc=1, device_id=(dom, peer), device_id_type=MESH)
    turn_maps(restrict_ref, wide_ref, turned_ref)
    pack_messages(turned_ref, list_ref, message_ref)
    pl.semaphore_wait(barrier, PEERS + SUBS - 1)
    copies = []
    for r, offset in enumerate(OFFSETS):
        peer = lax.rem(dom - offset + doms, doms)
        copies.append(
            pltpu.make_async_remote_copy(
                src_ref=message_ref.at[r], dst_ref=landed_ref.at[r],
                send_sem=send_sem.at[r], recv_sem=recv_sem.at[r],
                device_id=(peer, sub), device_id_type=MESH,
            )
        )
    for step in range(1, SUBS):
        peer = lax.rem(sub + step, subs)
        copies.append(
            pltpu.make_async_remote_copy(
                src_ref=coarse_ref, dst_ref=gathered_ref.at[step - 1],
                send_sem=map_send.at[step - 1], recv_sem=map_recv.at[step - 1],
                device_id=(dom, peer), device_id_type=MESH,
            )
        )
    for copy in copies:
        copy.start()
    maps_ref[0] = coarse_ref[...]
    for copy in copies:
        copy.wait()
    halo_ref[...] = landed_ref[...]
    for step in range(1, SUBS):
        maps_ref[step] = gathered_ref[step - 1]


def send_call(restrict1, send_list, coarse_pack):
    vmem = pl.BlockSpec(memory_space=pltpu.VMEM)
    return pl.pallas_call(
        send_kernel,
        name="send",
        out_shape=(
            jax.ShapeDtypeStruct((ROWS, LANES), BF16),
            jax.ShapeDtypeStruct((PEERS, QUARTER, LANES), BF16),
            jax.ShapeDtypeStruct((SUBS, LANES, LANES), F32),
        ),
        in_specs=[vmem] * 3,
        out_specs=(vmem,) * 3,
        scratch_shapes=[
            pltpu.VMEM((PAD * PITCH, LANES), F32),
            pltpu.VMEM((PEERS, QUARTER, LANES), BF16),
            pltpu.VMEM((PEERS, QUARTER, LANES), BF16),
            pltpu.VMEM((SUBS - 1, LANES, LANES), F32),
            pltpu.SemaphoreType.DMA((PEERS,)),
            pltpu.SemaphoreType.DMA((PEERS,)),
            pltpu.SemaphoreType.DMA((SUBS - 1,)),
            pltpu.SemaphoreType.DMA((SUBS - 1,)),
        ],
        compiler_params=pltpu.CompilerParams(collective_id=0, has_side_effects=True),
    )(restrict1, send_list, coarse_pack)


def main_kernel(
    turned_ref, halo_ref, maps_ref, face_ref, diag_ref, link_ref, slot_ref, group_ref,
    level_ref, owner_ref, far_ref, place_ref,
    one_ref, two_ref,
    wide_ref, near_ref, half_ref, mask_ref, member_ref, left_ref, right_ref,
    coarse_ref, high_ref, low_ref, band_ref, block_high, block_low, mixed_ref,
):
    def widen(k, carry):
        for i in range(NB):
            wide_ref[k, i, pl.ds(0, NB), :] = face_ref[k, i].astype(F32)
        return carry

    lax.fori_loop(0, FACES, widen, 0)
    for i in range(NB):
        wide_ref[FACES, i, pl.ds(0, NB), :] = diag_ref[i].astype(F32)
    near_ref[FACES] = turned_ref[...].astype(F32)

    links = jnp.concatenate([link_ref[pl.ds(k, 1), :] for k in range(FACES)], axis=1)
    pick = (iota((3 * LANES, FACES * LANES), 0) == links).astype(BF16)
    source = iota((PEERS * LANES, 2 * LANES), 0)
    target = iota((PEERS * LANES, 2 * LANES), 1)
    landing = (source // LANES) * HALO + source % HALO == target
    letters = jnp.concatenate([halo_ref[r] for r in range(PEERS)], axis=1)
    for q in range(GROUPS):
        unpack = (landing & ((source % LANES) // HALO == q)).astype(BF16)
        far = dot(letters, unpack).astype(BF16)
        rows = jnp.concatenate([turned_ref[pl.ds(q * QUARTER, QUARTER), :], far], axis=1)
        found = dot(rows, pick)
        for k in range(FACES):
            near_ref[k, pl.ds(q * QUARTER, QUARTER), :] = found[:, k * LANES : (k + 1) * LANES]

    block = 5
    blocks = NB // block

    def product(step, carry):
        k = step // blocks
        first = (step % blocks) * block
        total = [[None] * 4 for _ in range(block)]
        for m in range(NB):
            tiles = [near_ref[k, pl.ds(m * PAD + 8 * t, 8), :] for t in range(4)]
            for i in range(block):
                row = wide_ref[k, first + i, pl.ds(m, 8, stride=0), :]
                for t in range(4):
                    term = row * tiles[t]
                    total[i][t] = term if m == 0 else total[i][t] + term
        for i in range(block):
            half_ref[k, first + i] = jnp.concatenate(total[i], axis=0).astype(BF16)
        return carry

    lax.fori_loop(0, (FACES + 1) * blocks, product, 0)

    for k in range(FACES):
        row = jnp.broadcast_to(slot_ref[pl.ds(k, 1), :], (16, LANES))
        for j in range(SLOTS):
            mask_ref[k * SLOTS + j] = jnp.where(row == j, 1.0, 0.0).astype(BF16)
    group = jnp.broadcast_to(group_ref[...], (16, LANES))
    for g in range(AGGS):
        member_ref[g] = jnp.where(group == g, 1.0, 0.0).astype(BF16)

    def gather_slots(i, carry):
        column = pl.ds(pl.multiple_of(i * LANES, LANES), LANES)
        for part in range(2):
            span = pl.ds(16 * part, 16)
            half = [half_ref[k, i, span, :] for k in range(FACES + 1)]
            for j in range(SLOTS):
                total = half[0] * mask_ref[j]
                for k in range(1, FACES):
                    total = total + half[k] * mask_ref[k * SLOTS + j]
                if j == 0:
                    total = total + half[FACES]
                right_ref[pl.ds(j * PAD + 16 * part, 16), column] = total
            tile = turned_ref[pl.ds(pl.multiple_of(i * PAD, PAD) + 16 * part, 16), :]
            for g in range(AGGS):
                left_ref[pl.ds(g * PAD + 16 * part, 16), column] = tile * member_ref[g]
        return carry

    lax.fori_loop(0, NB, gather_slots, 0)
    coarse_ref[...] = lax.dot_general(
        left_ref[...], right_ref[...], (((1,), (1,)), ((), ())), preferred_element_type=F32
    )
    for g in range(AGGS):
        for j in range(SLOTS):
            one_ref[j, pl.ds(g, NB, stride=AGGS), :] = coarse_ref[
                pl.ds(g * PAD, NB), pl.ds(j * PAD, NB)
            ]

    from_lane = iota((LANES, 2 * LANES), 0)
    to_lane = iota((LANES, 2 * LANES), 1)
    for q in range(GROUPS):
        spread = ((from_lane // PAD == q) & (from_lane % PAD == to_lane % PAD)).astype(BF16)
        for s in range(SUBS):
            high, low = split(maps_ref[s])
            rows = pl.ds((s * GROUPS + q) * LANES, LANES)
            high_ref[rows, :] = dot(high, spread).astype(BF16)
            low_ref[rows, :] = dot(low, spread).astype(BF16)
    band = iota((PAD, 2 * LANES), 1) // PAD
    for t in range(SLOTS):
        band_ref[t] = jnp.where(band == t, 1.0, 0.0).astype(BF16)
    sub = lax.axis_index("sub")

    def apply_maps(g, carry):
        for j in range(SLOTS):
            far = far_ref[j, g]
            owner = lax.rem(sub - far // AGGS + SUBS, SUBS)
            rows = pl.ds(pl.multiple_of((owner * AGGS + far % AGGS) * PAD, PAD), PAD)
            band = band_ref[place_ref[j, g]]
            block_high[pl.ds(j * PAD, PAD), :] = high_ref[rows, :] * band
            block_low[pl.ds(j * PAD, PAD), :] = low_ref[rows, :] * band
        rows = pl.ds(pl.multiple_of(g * PAD, PAD), PAD)
        high, low = split(coarse_ref[rows, :])
        both = dot(jnp.concatenate([high, low], axis=0), block_high[...])
        mixed_ref[rows, :] = both[:PAD] + both[PAD:] + dot(high, block_low[...])
        return carry

    lax.fori_loop(0, AGGS, apply_maps, 0)
    high, low = split(level_ref[...])
    owner = owner_ref[...]
    picks = [jnp.where(owner == c, 1.0, 0.0).astype(BF16) for c in range(SLOTS)]
    left_high = jnp.concatenate([high * p for p in picks], axis=0)
    left_low = jnp.concatenate([low * p for p in picks], axis=0)
    right_high, right_low = split(mixed_ref[...])
    two_ref[...] = dot(left_high, right_high) + (dot(left_low, right_high) + dot(left_high, right_low))


def main_call(turned, halo, maps, face_block, diag_block, neighbour, face_slot, agg_map, level, owner, coarse_nbr, coarse_slot):
    vmem = pl.BlockSpec(memory_space=pltpu.VMEM)
    smem = pl.BlockSpec(memory_space=pltpu.SMEM)
    wide = 2 * LANES
    return pl.pallas_call(
        main_kernel,
        name="galerkin",
        out_shape=(
            jax.ShapeDtypeStruct((SLOTS, NB * AGGS, NB), F32),
            jax.ShapeDtypeStruct((SLOTS * PAD, wide), F32),
        ),
        in_specs=[vmem] * 10 + [smem] * 2,
        out_specs=(vmem, vmem),
        scratch_shapes=[
            pltpu.VMEM((FACES + 1, NB, PAD, LANES), F32),
            pltpu.VMEM((FACES + 1, ROWS, LANES), F32),
            pltpu.VMEM((FACES + 1, NB, PAD, LANES), BF16),
            pltpu.VMEM((FACES * SLOTS, 16, LANES), BF16),
            pltpu.VMEM((AGGS, 16, LANES), BF16),
            pltpu.VMEM((AGGS * PAD, NB * LANES), BF16),
            pltpu.VMEM((SLOTS * PAD, NB * LANES), BF16),
            pltpu.VMEM((AGGS * PAD, wide), F32),
            pltpu.VMEM((SUBS * AGGS * PAD, wide), BF16),
            pltpu.VMEM((SUBS * AGGS * PAD, wide), BF16),
            pltpu.VMEM((SLOTS, PAD, wide), BF16),
            pltpu.VMEM((SLOTS * PAD, wide), BF16),
            pltpu.VMEM((SLOTS * PAD, wide), BF16),
            pltpu.VMEM((AGGS * PAD, wide), F32),
        ],
        compiler_params=pltpu.CompilerParams(vmem_limit_bytes=56 * 2**20),
    )(turned, halo, maps, face_block, diag_block, neighbour, face_slot, agg_map, level, owner, coarse_nbr, coarse_slot)


def share_kernel(part_ref, sum_ref, landed_ref, send_sem, recv_sem):
    dom, sub = lax.axis_index("dom"), lax.axis_index("sub")
    subs = lax.axis_size("sub")
    rows = 2 * PAD
    barrier = pltpu.get_barrier_semaphore()
    for step in range(1, SUBS):
        peer = lax.rem(sub + step, subs)
        pl.semaphore_signal(barrier, inc=1, device_id=(dom, peer), device_id_type=MESH)
    pl.semaphore_wait(barrier, SUBS - 1)
    copies = []
    for step in range(1, SUBS):
        peer = lax.rem(sub + step, subs)
        copies.append(
            pltpu.make_async_remote_copy(
                src_ref=part_ref.at[pl.ds(pl.multiple_of(peer * rows, rows), rows), :],
                dst_ref=landed_ref.at[step - 1],
                send_sem=send_sem.at[step - 1], recv_sem=recv_sem.at[step - 1],
                device_id=(dom, peer), device_id_type=MESH,
            )
        )
    for copy in copies:
        copy.start()
    for copy in copies:
        copy.wait()
    own = part_ref[pl.ds(pl.multiple_of(sub * rows, rows), rows), :]
    sum_ref[...] = (own + landed_ref[0]) + (landed_ref[1] + landed_ref[2])


def share_call(part):
    vmem = pl.BlockSpec(memory_space=pltpu.VMEM)
    shape = (2 * PAD, 2 * LANES)
    return pl.pallas_call(
        share_kernel,
        name="share",
        out_shape=jax.ShapeDtypeStruct(shape, F32),
        in_specs=[vmem],
        out_specs=vmem,
        scratch_shapes=[
            pltpu.VMEM((SUBS - 1,) + shape, F32),
            pltpu.SemaphoreType.DMA((SUBS - 1,)),
            pltpu.SemaphoreType.DMA((SUBS - 1,)),
        ],
        compiler_params=pltpu.CompilerParams(collective_id=1, has_side_effects=True),
    )(part)


def pack_level(restrict2, agg2_map):
    padded = jnp.pad(restrict2, ((0, 2), (0, 2), (0, 0)))
    pack = padded.reshape(PAD, PAD, GROUPS, GROUPS).transpose(3, 1, 2, 0).reshape(LANES, LANES)
    level = padded.transpose(0, 2, 1).reshape(PAD, AGGS * PAD)
    owner = jnp.repeat(agg2_map, PAD).reshape(1, AGGS * PAD)
    return pack, level, owner


def per_device(
    diag_block, face_block, restrict1, neighbour, face_slot, agg_map,
    send_list, restrict2, coarse_nbr, agg2_map, coarse_slot,
):
    pack, level, owner = pack_level(restrict2, agg2_map)
    turned, halo, maps = send_call(restrict1, send_list, pack)
    one, part = main_call(
        turned, halo, maps, face_block, diag_block, neighbour, face_slot,
        agg_map.reshape(1, LANES), level, owner, coarse_nbr, coarse_slot,
    )
    total = share_call(part)
    one = one.reshape(SLOTS, NB, AGGS, NB).transpose(0, 1, 3, 2)
    two = total.reshape(2, PAD, SLOTS, PAD)[:, :NB, :, :NB].transpose(2, 1, 3, 0)
    return one, two


def solution(mesh):
    both = ("dom", "sub")
    placed = (
        P(None, None, both), P(None, None, None, both), P(None, None, both),
        P(None, both), P(None, both), P(both), P(None, both),
        P(None, None, both), P(None, both), P(both), P(None, both),
    )
    return jax.shard_map(
        per_device,
        mesh=mesh,
        in_specs=placed,
        out_specs=(P(None, None, None, both), P(None, None, None, both)),
        check_vma=False,
    )
```

```python
import jax
import jax.numpy as jnp
from jax import lax
from jax.experimental import pallas as pl
from jax.experimental.pallas import tpu as pltpu
from jax.sharding import PartitionSpec as P

NB = 30
PAD = 32
PITCH = 40
LANES = 128
FACES = 6
SLOTS = 8
HALO = 32
REACH = 3
PEERS = 6
GROUPS = 4
ROWS = NB * PAD
QUARTER = ROWS // GROUPS
AGGS = 16
SUBS = 4
F32 = jnp.float32
BF16 = jnp.bfloat16
MESH = pl.DeviceIdType.MESH
OFFSETS = tuple(r - REACH if r < REACH else r - REACH + 1 for r in range(PEERS))


def iota(shape, dim):
    return lax.broadcasted_iota(jnp.int32, shape, dim)


def dot(a, b):
    return jnp.dot(a, b, preferred_element_type=F32)


def split(x):
    high = x.astype(BF16)
    return high, (x - high.astype(F32)).astype(BF16)


def turn_maps(restrict_ref, wide_ref, turned_ref):
    wide_ref[pl.ds(NB * PITCH, 2 * PITCH), :] = jnp.zeros((2 * PITCH, LANES), F32)
    for n in range(NB):
        wide_ref[pl.ds(n * PITCH, NB), :] = restrict_ref[n].astype(F32)
    for m in range(NB):
        turned_ref[pl.ds(m * PAD, PAD), :] = wide_ref[pl.ds(m, PAD, stride=PITCH), :].astype(BF16)


def pack_messages(turned_ref, list_ref, message_ref):
    lane_group = iota((QUARTER, LANES), 1) // HALO
    rows = turned_ref[...]
    for r in range(PEERS):
        row = list_ref[pl.ds(r, 1), :]
        four = jnp.concatenate([row] * GROUPS, axis=1)
        pick = (iota((LANES, LANES), 0) == four).astype(BF16)
        chosen = dot(rows, pick)
        packed = jnp.zeros((QUARTER, LANES), F32)
        for q in range(GROUPS):
            packed = jnp.where(lane_group == q, chosen[q * QUARTER : (q + 1) * QUARTER], packed)
        message_ref[r] = packed.astype(BF16)


def pack_level(level_ref, square_ref, pack_ref, coarse_ref):
    square_ref[...] = jnp.zeros(square_ref.shape, F32)
    square_ref[pl.ds(0, NB * AGGS), pl.ds(0, NB)] = level_ref[...]
    for low in range(GROUPS):
        pieces = [
            square_ref[pl.ds(q * GROUPS + low, PAD, stride=AGGS), :] for q in range(GROUPS)
        ]
        pack_ref[pl.ds(low * PAD, PAD), :] = jnp.concatenate(pieces, axis=1)
    coarse_ref[...] = pack_ref[...].T


def spread_maps(step, values, high_ref, low_ref):
    from_lane = iota((LANES, 2 * LANES), 0)
    to_lane = iota((LANES, 2 * LANES), 1)
    high, low = split(values)
    for q in range(GROUPS):
        spread = ((from_lane // PAD == q) & (from_lane % PAD == to_lane % PAD)).astype(BF16)
        blocks = pl.ds((step * GROUPS + q) * GROUPS, GROUPS)
        shape = (GROUPS, PAD, 2 * LANES)
        high_ref[blocks] = dot(high, spread).astype(BF16).reshape(shape)
        low_ref[blocks] = dot(low, spread).astype(BF16).reshape(shape)


def product(k, step, near_ref, wide_ref, half_ref):
    block = 5
    first = step * block
    total = [[None] * 4 for _ in range(block)]
    for m in range(NB):
        tiles = [near_ref[k, pl.ds(m * PAD + 8 * t, 8), :] for t in range(4)]
        for i in range(block):
            row = wide_ref[k, first + i, pl.ds(m, 8, stride=0), :]
            for t in range(4):
                term = row * tiles[t]
                total[i][t] = term if m == 0 else total[i][t] + term
    for i in range(block):
        half_ref[k, first + i] = jnp.concatenate(total[i], axis=0).astype(BF16)


def kernel(
    restrict_ref, diag_ref, link_ref, slot_ref, group_ref, list_ref, level_ref,
    far_ref, place_ref, owner_ref, face_hbm,
    one_hbm, two_ref,
    tall_ref, turned_ref, message_ref, landed_ref, square_ref, pack_ref, coarse_ref, gathered_ref,
    face_ref, wide_ref, near_ref, half_ref, mask_ref, member_ref, left_ref, right_ref,
    one_ref, whole_ref, high_ref, low_ref, band_ref, block_high, block_low, mixed_ref,
    spot_ref, part_ref, arrived_ref,
    face_sem, one_sem, send_sem, recv_sem, map_send, map_recv, part_send, part_recv,
):
    dom, sub = lax.axis_index("dom"), lax.axis_index("sub")
    doms, subs = lax.axis_size("dom"), lax.axis_size("sub")
    face_copy = pltpu.make_async_copy(face_hbm, face_ref, face_sem)
    face_copy.start()
    barrier = pltpu.get_barrier_semaphore()
    for offset in OFFSETS:
        peer = lax.rem(dom + offset + doms, doms)
        pl.semaphore_signal(barrier, inc=1, device_id=(peer, sub), device_id_type=MESH)
    for step in range(1, SUBS):
        peer = lax.rem(sub + step, subs)
        pl.semaphore_signal(barrier, inc=1, device_id=(dom, peer), device_id_type=MESH)

    turn_maps(restrict_ref, tall_ref, turned_ref)
    pack_messages(turned_ref, list_ref, message_ref)
    pack_level(level_ref, square_ref, pack_ref, coarse_ref)
    pl.semaphore_wait(barrier, PEERS + SUBS - 1)

    halos, maps = [], []
    for r, offset in enumerate(OFFSETS):
        peer = lax.rem(dom - offset + doms, doms)
        halos.append(
            pltpu.make_async_remote_copy(
                src_ref=message_ref.at[r], dst_ref=landed_ref.at[r],
                send_sem=send_sem.at[r], recv_sem=recv_sem.at[r],
                device_id=(peer, sub), device_id_type=MESH,
            )
        )
    for step in range(1, SUBS):
        peer = lax.rem(sub + step, subs)
        maps.append(
            pltpu.make_async_remote_copy(
                src_ref=coarse_ref, dst_ref=gathered_ref.at[step - 1],
                send_sem=map_send.at[step - 1], recv_sem=map_recv.at[step - 1],
                device_id=(dom, peer), device_id_type=MESH,
            )
        )
    for copy in halos + maps:
        copy.start()

    for i in range(NB):
        wide_ref[FACES, i, pl.ds(0, NB), :] = diag_ref[i].astype(F32)
    near_ref[FACES] = turned_ref[...].astype(F32)

    def own_product(step, carry):
        product(FACES, step, near_ref, wide_ref, half_ref)
        return carry

    lax.fori_loop(0, NB // 5, own_product, 0)

    for k in range(FACES):
        row = jnp.broadcast_to(slot_ref[pl.ds(k, 1), :], (16, LANES))
        for j in range(SLOTS):
            mask_ref[k * SLOTS + j] = jnp.where(row == j, 1.0, 0.0).astype(BF16)
    group = jnp.broadcast_to(group_ref[...], (16, LANES))
    for g in range(AGGS):
        member_ref[g] = jnp.where(group == g, 1.0, 0.0).astype(BF16)

    def mask_left(i, carry):
        column = pl.ds(pl.multiple_of(i * LANES, LANES), LANES)
        for part in range(2):
            tile = turned_ref[pl.ds(pl.multiple_of(i * PAD, PAD) + 16 * part, 16), :]
            for g in range(AGGS):
                left_ref[pl.ds(g * PAD + 16 * part, 16), column] = tile * member_ref[g]
        return carry

    lax.fori_loop(0, NB, mask_left, 0)
    face_copy.wait()

    def widen(k, carry):
        for i in range(NB):
            wide_ref[k, i, pl.ds(0, NB), :] = face_ref[k, i].astype(F32)
        return carry

    lax.fori_loop(0, FACES, widen, 0)

    band = iota((PAD, 2 * LANES), 1) // PAD
    for t in range(SLOTS):
        band_ref[t] = jnp.where(band == t, 1.0, 0.0).astype(BF16)
    lane_agg = iota((PAD, AGGS * PAD), 1) // PAD
    owner = jnp.zeros((PAD, AGGS * PAD), jnp.int32)
    for g in range(AGGS):
        owner = jnp.where(lane_agg == (g % GROUPS) * GROUPS + g // GROUPS, owner_ref[0, g], owner)
    level = jnp.concatenate([pack_ref[pl.ds(x * PAD, PAD), :] for x in range(GROUPS)], axis=1)
    for c in range(SLOTS):
        rows = pl.ds((c // 2) * 2 * PAD + c % 2, PAD, stride=2)
        picked = jnp.where(owner == c, level, 0.0)
        for x in range(GROUPS):
            spot_ref[x, rows, :] = picked[:, x * LANES : (x + 1) * LANES]
    spread_maps(0, coarse_ref[...], high_ref, low_ref)
    for copy in maps:
        copy.wait()
    for step in range(1, SUBS):
        spread_maps(step, gathered_ref[step - 1], high_ref, low_ref)

    def place_blocks(g, carry):
        for j in range(SLOTS):
            far = far_ref[j, g]
            step = lax.rem(sub - lax.div(far, AGGS) + SUBS, SUBS)
            agg = lax.rem(far, AGGS)
            index = step * AGGS + lax.rem(agg, GROUPS) * GROUPS + lax.div(agg, GROUPS)
            mask = band_ref[place_ref[j, g]]
            block_high[g, pl.ds(j * PAD, PAD), :] = high_ref[index] * mask
            block_low[g, pl.ds(j * PAD, PAD), :] = low_ref[index] * mask
        return carry

    lax.fori_loop(0, AGGS, place_blocks, 0)

    links = jnp.concatenate([link_ref[pl.ds(k, 1), :] for k in range(FACES)], axis=1)
    pick = (iota((3 * LANES, FACES * LANES), 0) == links).astype(BF16)
    source = iota((PEERS * LANES, 2 * LANES), 0)
    target = iota((PEERS * LANES, 2 * LANES), 1)
    landing = (source // LANES) * HALO + source % HALO == target
    for copy in halos:
        copy.wait()
    letters = jnp.concatenate([landed_ref[r] for r in range(PEERS)], axis=1)
    for q in range(GROUPS):
        unpack = (landing & ((source % LANES) // HALO == q)).astype(BF16)
        far = dot(letters, unpack).astype(BF16)
        rows = jnp.concatenate([turned_ref[pl.ds(q * QUARTER, QUARTER), :], far], axis=1)
        found = dot(rows, pick)
        for k in range(FACES):
            near_ref[k, pl.ds(q * QUARTER, QUARTER), :] = found[:, k * LANES : (k + 1) * LANES]

    def face_product(index, carry):
        product(index // (NB // 5), index % (NB // 5), near_ref, wide_ref, half_ref)
        return carry

    lax.fori_loop(0, FACES * (NB // 5), face_product, 0)

    def gather_slots(pair, carry):
        for i in (2 * pair, 2 * pair + 1):
            column = pl.ds(pl.multiple_of(i * LANES, LANES), LANES)
            for part in range(2):
                span = pl.ds(16 * part, 16)
                half = [half_ref[k, i, span, :] for k in range(FACES + 1)]
                for j in range(SLOTS):
                    total = half[0] * mask_ref[j]
                    for k in range(1, FACES):
                        total = total + half[k] * mask_ref[k * SLOTS + j]
                    if j == 0:
                        total = total + half[FACES]
                    right_ref[pl.ds(j * PAD + 16 * part, 16), column] = total
        return carry

    lax.fori_loop(0, NB // 2, gather_slots, 0)
    whole_ref[...] = lax.dot_general(
        left_ref[...], right_ref[...], (((1,), (1,)), ((), ())), preferred_element_type=F32
    )

    for g in range(AGGS):
        high, low = split(whole_ref[pl.ds(g * PAD, PAD), :])
        both = dot(jnp.concatenate([high, low], axis=0), block_high[g])
        rows = pl.ds(((g % GROUPS) * GROUPS + g // GROUPS) * PAD, PAD)
        mixed_ref[rows, :] = both[:PAD] + both[PAD:] + dot(high, block_low[g])
    left_high, left_low = split(jnp.concatenate([spot_ref[x] for x in range(GROUPS)], axis=1))
    right_high, right_low = split(mixed_ref[...])
    part_ref[...] = dot(left_high, right_high) + (dot(left_low, right_high) + dot(left_high, right_low))

    def lay_out(aggs):
        for g in aggs:
            for j in range(SLOTS):
                one_ref[j, pl.ds(g, NB, stride=AGGS), :] = whole_ref[
                    pl.ds(g * PAD, NB), pl.ds(j * PAD, NB)
                ]

    lay_out(range(4))
    rows = 2 * PAD
    parts = []
    for step in range(1, SUBS):
        peer = lax.rem(sub + step, subs)
        parts.append(
            pltpu.make_async_remote_copy(
                src_ref=part_ref.at[pl.ds(pl.multiple_of(peer * rows, rows), rows), :],
                dst_ref=arrived_ref.at[step - 1],
                send_sem=part_send.at[step - 1], recv_sem=part_recv.at[step - 1],
                device_id=(dom, peer), device_id_type=MESH,
            )
        )
    for copy in parts:
        copy.start()
    lay_out(range(4, AGGS))
    one_copy = pltpu.make_async_copy(one_ref, one_hbm, one_sem)
    one_copy.start()
    for copy in parts:
        copy.wait()
    own = part_ref[pl.ds(pl.multiple_of(sub * rows, rows), rows), :]
    total = (own + arrived_ref[0]) + (arrived_ref[1] + arrived_ref[2])
    for t in range(SLOTS):
        two_ref[pl.ds(t * 2 * NB, 2 * NB), :] = total[: 2 * NB, t * PAD : t * PAD + NB]
    one_copy.wait()


def fused_call(*arrays):
    vmem = pl.BlockSpec(memory_space=pltpu.VMEM)
    smem = pl.BlockSpec(memory_space=pltpu.SMEM)
    hbm = pl.BlockSpec(memory_space=pl.ANY)
    dma = pltpu.SemaphoreType.DMA
    wide = 2 * LANES
    one_shape = (SLOTS, NB * AGGS, NB)
    return pl.pallas_call(
        kernel,
        name="galerkin",
        out_shape=(
            jax.ShapeDtypeStruct(one_shape, F32),
            jax.ShapeDtypeStruct((SLOTS * 2 * NB, NB), F32),
        ),
        in_specs=[vmem] * 7 + [smem] * 3 + [hbm],
        out_specs=(hbm, vmem),
        scratch_shapes=[
            pltpu.VMEM((PAD * PITCH, LANES), F32),
            pltpu.VMEM((ROWS, LANES), BF16),
            pltpu.VMEM((PEERS, QUARTER, LANES), BF16),
            pltpu.VMEM((PEERS, QUARTER, LANES), BF16),
            pltpu.VMEM((PAD * AGGS, PAD), F32),
            pltpu.VMEM((LANES, LANES), F32),
            pltpu.VMEM((LANES, LANES), F32),
            pltpu.VMEM((SUBS - 1, LANES, LANES), F32),
            pltpu.VMEM((FACES, NB, NB, LANES), BF16),
            pltpu.VMEM((FACES + 1, NB, PAD, LANES), F32),
            pltpu.VMEM((FACES + 1, ROWS, LANES), F32),
            pltpu.VMEM((FACES + 1, NB, PAD, LANES), BF16),
            pltpu.VMEM((FACES * SLOTS, 16, LANES), BF16),
            pltpu.VMEM((AGGS, 16, LANES), BF16),
            pltpu.VMEM((AGGS * PAD, NB * LANES), BF16),
            pltpu.VMEM((SLOTS * PAD, NB * LANES), BF16),
            pltpu.VMEM(one_shape, F32),
            pltpu.VMEM((AGGS * PAD, wide), F32),
            pltpu.VMEM((SUBS * AGGS, PAD, wide), BF16),
            pltpu.VMEM((SUBS * AGGS, PAD, wide), BF16),
            pltpu.VMEM((SLOTS, PAD, wide), BF16),
            pltpu.VMEM((AGGS, SLOTS * PAD, wide), BF16),
            pltpu.VMEM((AGGS, SLOTS * PAD, wide), BF16),
            pltpu.VMEM((AGGS * PAD, wide), F32),
            pltpu.VMEM((GROUPS, SLOTS * PAD, LANES), F32),
            pltpu.VMEM((SLOTS * PAD, wide), F32),
            pltpu.VMEM((SUBS - 1, 2 * PAD, wide), F32),
            dma, dma,
            dma((PEERS,)), dma((PEERS,)),
            dma((SUBS - 1,)), dma((SUBS - 1,)),
            dma((SUBS - 1,)), dma((SUBS - 1,)),
        ],
        compiler_params=pltpu.CompilerParams(
            collective_id=0, has_side_effects=True, vmem_limit_bytes=62 * 2**20
        ),
    )(*arrays)


def per_device(
    diag_block, face_block, restrict1, neighbour, face_slot, agg_map,
    send_list, restrict2, coarse_nbr, agg2_map, coarse_slot,
):
    level = restrict2.transpose(0, 2, 1).reshape(NB * AGGS, NB)
    one, two = fused_call(
        restrict1, diag_block, neighbour, face_slot, agg_map.reshape(1, LANES), send_list, level,
        coarse_nbr, coarse_slot, agg2_map.reshape(1, AGGS), face_block,
    )
    one = one.reshape(SLOTS, NB, AGGS, NB).transpose(0, 1, 3, 2)
    two = two.reshape(SLOTS, NB, 2, NB).transpose(0, 1, 3, 2)
    return one, two


def solution(mesh):
    both = ("dom", "sub")
    placed = (
        P(None, None, both), P(None, None, None, both), P(None, None, both),
        P(None, both), P(None, both), P(both), P(None, both),
        P(None, None, both), P(None, both), P(both), P(None, both),
    )
    return jax.shard_map(
        per_device,
        mesh=mesh,
        in_specs=placed,
        out_specs=(P(None, None, None, both), P(None, None, None, both)),
        check_vma=False,
    )
```

```python
import jax
import jax.numpy as jnp
from jax import lax
from jax.experimental import pallas as pl
from jax.experimental.pallas import tpu as pltpu
from jax.sharding import PartitionSpec as P

NB = 30
PAD = 32
PITCH = 40
LANES = 128
FACES = 6
SLOTS = 8
HALO = 32
REACH = 3
PEERS = 6
GROUPS = 4
ROWS = NB * PAD
QUARTER = ROWS // GROUPS
AGGS = 16
SUBS = 4
F32 = jnp.float32
BF16 = jnp.bfloat16
MESH = pl.DeviceIdType.MESH
OFFSETS = tuple(r - REACH if r < REACH else r - REACH + 1 for r in range(PEERS))


def iota(shape, dim):
    return lax.broadcasted_iota(jnp.int32, shape, dim)


def dot(a, b):
    return jnp.dot(a, b, preferred_element_type=F32)


def split(x):
    high = x.astype(BF16)
    return high, (x - high.astype(F32)).astype(BF16)


def turn_maps(restrict_ref, wide_ref, turned_ref):
    wide_ref[pl.ds(NB * PITCH, 2 * PITCH), :] = jnp.zeros((2 * PITCH, LANES), F32)
    for n in range(NB):
        wide_ref[pl.ds(n * PITCH, NB), :] = restrict_ref[n].astype(F32)
    for m in range(NB):
        turned_ref[pl.ds(m * PAD, PAD), :] = wide_ref[pl.ds(m, PAD, stride=PITCH), :].astype(BF16)


def pack_messages(turned_ref, list_ref, message_ref):
    lane_group = iota((QUARTER, LANES), 1) // HALO
    rows = turned_ref[...]
    for r in range(PEERS):
        row = list_ref[pl.ds(r, 1), :]
        four = jnp.concatenate([row] * GROUPS, axis=1)
        pick = (iota((LANES, LANES), 0) == four).astype(BF16)
        chosen = dot(rows, pick)
        packed = jnp.zeros((QUARTER, LANES), F32)
        for q in range(GROUPS):
            packed = jnp.where(lane_group == q, chosen[q * QUARTER : (q + 1) * QUARTER], packed)
        message_ref[r] = packed.astype(BF16)


def pack_level(level_ref, square_ref, pack_ref, coarse_ref):
    square_ref[...] = jnp.zeros(square_ref.shape, F32)
    square_ref[pl.ds(0, NB * AGGS), pl.ds(0, NB)] = level_ref[...]
    for low in range(GROUPS):
        pieces = [
            square_ref[pl.ds(q * GROUPS + low, PAD, stride=AGGS), :] for q in range(GROUPS)
        ]
        pack_ref[pl.ds(low * PAD, PAD), :] = jnp.concatenate(pieces, axis=1)
    coarse_ref[...] = pack_ref[...].T


def spread_maps(step, values, high_ref, low_ref):
    from_lane = iota((LANES, 2 * LANES), 0)
    to_lane = iota((LANES, 2 * LANES), 1)
    high, low = split(values)
    for q in range(GROUPS):
        spread = ((from_lane // PAD == q) & (from_lane % PAD == to_lane % PAD)).astype(BF16)
        blocks = pl.ds((step * GROUPS + q) * GROUPS, GROUPS)
        shape = (GROUPS, PAD, 2 * LANES)
        high_ref[blocks] = dot(high, spread).astype(BF16).reshape(shape)
        low_ref[blocks] = dot(low, spread).astype(BF16).reshape(shape)


def product(k, step, near_ref, wide_ref, half_ref):
    block = 5
    first = step * block
    total = [[None] * 4 for _ in range(block)]
    for m in range(NB):
        tiles = [near_ref[pl.ds(m * PAD + 8 * t, 8), :] for t in range(4)]
        for i in range(block):
            row = wide_ref[k, first + i, pl.ds(m, 8, stride=0), :]
            for t in range(4):
                term = row * tiles[t]
                total[i][t] = term if m == 0 else total[i][t] + term
    for i in range(block):
        half_ref[k, first + i] = jnp.concatenate(total[i], axis=0).astype(BF16)


def kernel(
    restrict_hbm, diag_hbm, link_hbm, slot_hbm, group_hbm, list_hbm, level_hbm,
    far_hbm, place_hbm, owner_hbm, face_hbm,
    one_ref, two_ref,
    restrict_ref, diag_ref, link_ref, slot_ref, group_ref, list_ref, level_ref,
    far_ref, place_ref, owner_ref,
    tall_ref, turned_ref, message_ref, landed_ref, square_ref, pack_ref, coarse_ref, gathered_ref,
    face_ref, wide_ref, near_even, near_odd, half_ref, mask_ref, member_ref, left_ref, right_ref,
    pick_ref, unpack_ref, extended_ref, whole_ref, high_ref, low_ref, band_ref, block_high, block_low, mixed_ref,
    spot_ref, part_ref, small_ref, arrived_ref,
    load_sem, send_sem, recv_sem, map_send, map_recv, part_send, part_recv,
):
    dom, sub = lax.axis_index("dom"), lax.axis_index("sub")
    doms, subs = lax.axis_size("dom"), lax.axis_size("sub")
    barrier = pltpu.get_barrier_semaphore()
    for offset in OFFSETS:
        peer = lax.rem(dom + offset + doms, doms)
        pl.semaphore_signal(barrier, inc=1, device_id=(peer, sub), device_id_type=MESH)
    for step in range(1, SUBS):
        peer = lax.rem(sub + step, subs)
        pl.semaphore_signal(barrier, inc=1, device_id=(dom, peer), device_id_type=MESH)

    loads = [
        pltpu.make_async_copy(source, target, load_sem.at[x])
        for x, (source, target) in enumerate(
            (
                (restrict_hbm, restrict_ref), (list_hbm, list_ref), (level_hbm, level_ref),
                (diag_hbm, diag_ref), (link_hbm, link_ref), (slot_hbm, slot_ref),
                (group_hbm, group_ref), (owner_hbm, owner_ref), (far_hbm, far_ref),
                (place_hbm, place_ref), (face_hbm, face_ref),
            )
        )
    ]
    for load in loads:
        load.start()
    loads[0].wait()
    turn_maps(restrict_ref, tall_ref, turned_ref)
    loads[1].wait()
    pack_messages(turned_ref, list_ref, message_ref)
    pl.semaphore_wait(barrier, PEERS + SUBS - 1)

    halos, maps = [], []
    for r, offset in enumerate(OFFSETS):
        peer = lax.rem(dom - offset + doms, doms)
        halos.append(
            pltpu.make_async_remote_copy(
                src_ref=message_ref.at[r], dst_ref=landed_ref.at[r],
                send_sem=send_sem.at[r], recv_sem=recv_sem.at[r],
                device_id=(peer, sub), device_id_type=MESH,
            )
        )
    for step in range(1, SUBS):
        peer = lax.rem(sub + step, subs)
        maps.append(
            pltpu.make_async_remote_copy(
                src_ref=coarse_ref, dst_ref=gathered_ref.at[step - 1],
                send_sem=map_send.at[step - 1], recv_sem=map_recv.at[step - 1],
                device_id=(dom, peer), device_id_type=MESH,
            )
        )
    for copy in halos:
        copy.start()
    loads[2].wait()
    pack_level(level_ref, square_ref, pack_ref, coarse_ref)

    for load in loads[3:10]:
        load.wait()
    for i in range(NB):
        wide_ref[FACES, i, pl.ds(0, NB), :] = diag_ref[i].astype(F32)
    near_odd[...] = turned_ref[...].astype(F32)

    def own_product(step, carry):
        product(FACES, step, near_odd, wide_ref, half_ref)
        return carry

    lax.fori_loop(0, NB // 5, own_product, 0)
    for copy in maps:
        copy.start()

    for k in range(FACES):
        row = jnp.broadcast_to(slot_ref[pl.ds(k, 1), :], (16, LANES))
        for j in range(SLOTS):
            mask_ref[k * SLOTS + j] = jnp.where(row == j, 1.0, 0.0).astype(BF16)
    group = jnp.broadcast_to(group_ref[...], (16, LANES))
    for g in range(AGGS):
        member_ref[g] = jnp.where(group == g, 1.0, 0.0).astype(BF16)

    def mask_left(i, carry):
        column = pl.ds(pl.multiple_of(i * LANES, LANES), LANES)
        for part in range(2):
            tile = turned_ref[pl.ds(pl.multiple_of(i * PAD, PAD) + 16 * part, 16), :]
            for g in range(AGGS):
                left_ref[pl.ds(g * PAD + 16 * part, 16), column] = tile * member_ref[g]
        return carry

    lax.fori_loop(0, NB, mask_left, 0)
    loads[10].wait()

    def widen(k, carry):
        for i in range(NB):
            wide_ref[k, i, pl.ds(0, NB), :] = face_ref[k, i].astype(F32)
        return carry

    lax.fori_loop(0, FACES, widen, 0)

    band = iota((PAD, 2 * LANES), 1) // PAD
    for t in range(SLOTS):
        band_ref[t] = jnp.where(band == t, 1.0, 0.0).astype(BF16)
    lane_agg = iota((PAD, AGGS * PAD), 1) // PAD
    owner = jnp.zeros((PAD, AGGS * PAD), jnp.int32)
    for g in range(AGGS):
        owner = jnp.where(lane_agg == (g % GROUPS) * GROUPS + g // GROUPS, owner_ref[0, g], owner)
    level = jnp.concatenate([pack_ref[pl.ds(x * PAD, PAD), :] for x in range(GROUPS)], axis=1)
    for c in range(SLOTS):
        rows = pl.ds((c // 2) * 2 * PAD + c % 2, PAD, stride=2)
        picked = jnp.where(owner == c, level, 0.0)
        for x in range(GROUPS):
            spot_ref[x, rows, :] = picked[:, x * LANES : (x + 1) * LANES]
    spread_maps(0, coarse_ref[...], high_ref, low_ref)
    for copy in maps:
        copy.wait()
    for step in range(1, SUBS):
        spread_maps(step, gathered_ref[step - 1], high_ref, low_ref)

    def place_blocks(g, carry):
        for j in range(SLOTS):
            far = far_ref[j, g]
            step = lax.rem(sub - lax.div(far, AGGS) + SUBS, SUBS)
            agg = lax.rem(far, AGGS)
            index = step * AGGS + lax.rem(agg, GROUPS) * GROUPS + lax.div(agg, GROUPS)
            mask = band_ref[place_ref[j, g]]
            block_high[g, pl.ds(j * PAD, PAD), :] = high_ref[index] * mask
            block_low[g, pl.ds(j * PAD, PAD), :] = low_ref[index] * mask
        return carry

    lax.fori_loop(0, AGGS, place_blocks, 0)

    for k in range(FACES):
        pick_ref[k] = (iota((3 * LANES, LANES), 0) == link_ref[pl.ds(k, 1), :]).astype(BF16)
    source = iota((PEERS * LANES, 2 * LANES), 0)
    target = iota((PEERS * LANES, 2 * LANES), 1)
    landing = (source // LANES) * HALO + source % HALO == target
    for q in range(GROUPS):
        unpack_ref[q] = (landing & ((source % LANES) // HALO == q)).astype(BF16)
    extended_ref[:, pl.ds(0, LANES)] = turned_ref[...]
    for copy in halos:
        copy.wait()

    letters = jnp.concatenate([landed_ref[r] for r in range(PEERS)], axis=1)
    for q in range(GROUPS):
        far = dot(letters, unpack_ref[q]).astype(BF16)
        extended_ref[pl.ds(q * QUARTER, QUARTER), pl.ds(LANES, 2 * LANES)] = far
    near_even[...] = dot(extended_ref[...], pick_ref[0])

    steps = NB // 5
    for k in range(FACES):
        now, later = (near_even, near_odd) if k % 2 == 0 else (near_odd, near_even)

        def face_product(step, carry, k=k, now=now, later=later):
            if k + 1 < FACES:
                rows = pl.ds(pl.multiple_of(step * 5 * PAD, 5 * PAD), 5 * PAD)
                later[rows, :] = dot(extended_ref[rows, :], pick_ref[k + 1])
            product(k, step, now, wide_ref, half_ref)
            return carry

        lax.fori_loop(0, steps, face_product, 0)

    def gather_slots(pair, carry):
        for i in (2 * pair, 2 * pair + 1):
            column = pl.ds(pl.multiple_of(i * LANES, LANES), LANES)
            for part in range(2):
                span = pl.ds(16 * part, 16)
                half = [half_ref[k, i, span, :] for k in range(FACES + 1)]
                for j in range(SLOTS):
                    total = half[0] * mask_ref[j]
                    for k in range(1, FACES):
                        total = total + half[k] * mask_ref[k * SLOTS + j]
                    if j == 0:
                        total = total + half[FACES]
                    right_ref[pl.ds(j * PAD + 16 * part, 16), column] = total
        return carry

    lax.fori_loop(0, NB // 2, gather_slots, 0)
    whole_ref[...] = lax.dot_general(
        left_ref[...], right_ref[...], (((1,), (1,)), ((), ())), preferred_element_type=F32
    )

    for g in range(AGGS):
        high, low = split(whole_ref[pl.ds(g * PAD, PAD), :])
        both = dot(jnp.concatenate([high, low], axis=0), block_high[g])
        rows = pl.ds(((g % GROUPS) * GROUPS + g // GROUPS) * PAD, PAD)
        mixed_ref[rows, :] = both[:PAD] + both[PAD:] + dot(high, block_low[g])
    left_high, left_low = split(jnp.concatenate([spot_ref[x] for x in range(GROUPS)], axis=1))
    right_high, right_low = split(mixed_ref[...])
    part = dot(left_high, right_high) + (dot(left_low, right_high) + dot(left_high, right_low))
    part_ref[...] = part
    small_ref[...] = part.astype(BF16)

    def lay_out(aggs):
        for g in aggs:
            for j in range(SLOTS):
                one_ref[j, pl.ds(g, NB, stride=AGGS), :] = whole_ref[
                    pl.ds(g * PAD, NB), pl.ds(j * PAD, NB)
                ]

    lay_out(range(4))
    rows = 2 * PAD
    parts = []
    for step in range(1, SUBS):
        peer = lax.rem(sub + step, subs)
        parts.append(
            pltpu.make_async_remote_copy(
                src_ref=small_ref.at[pl.ds(pl.multiple_of(peer * rows, rows), rows), :],
                dst_ref=arrived_ref.at[step - 1],
                send_sem=part_send.at[step - 1], recv_sem=part_recv.at[step - 1],
                device_id=(dom, peer), device_id_type=MESH,
            )
        )
    for copy in parts:
        copy.start()
    lay_out(range(4, AGGS))
    for copy in parts:
        copy.wait()
    own = part_ref[pl.ds(pl.multiple_of(sub * rows, rows), rows), :]
    others = [arrived_ref[x].astype(F32) for x in range(SUBS - 1)]
    total = (own + others[0]) + (others[1] + others[2])
    for t in range(SLOTS):
        two_ref[pl.ds(t * 2 * NB, 2 * NB), :] = total[: 2 * NB, t * PAD : t * PAD + NB]


def fused_call(*arrays):
    vmem = pl.BlockSpec(memory_space=pltpu.VMEM)
    hbm = pl.BlockSpec(memory_space=pltpu.HBM)
    dma = pltpu.SemaphoreType.DMA
    wide = 2 * LANES
    one_shape = (SLOTS, NB * AGGS, NB)
    return pl.pallas_call(
        kernel,
        name="galerkin",
        out_shape=(
            jax.ShapeDtypeStruct(one_shape, F32),
            jax.ShapeDtypeStruct((SLOTS * 2 * NB, NB), F32),
        ),
        in_specs=[hbm] * 11,
        out_specs=(vmem, vmem),
        scratch_shapes=[
            pltpu.VMEM((NB, NB, LANES), BF16),
            pltpu.VMEM((NB, NB, LANES), BF16),
            pltpu.VMEM((FACES, LANES), jnp.int32),
            pltpu.VMEM((FACES, LANES), jnp.int32),
            pltpu.VMEM((1, LANES), jnp.int32),
            pltpu.VMEM((PEERS, HALO), jnp.int32),
            pltpu.VMEM((NB * AGGS, NB), F32),
            pltpu.SMEM((SLOTS, AGGS), jnp.int32),
            pltpu.SMEM((SLOTS, AGGS), jnp.int32),
            pltpu.SMEM((1, AGGS), jnp.int32),
            pltpu.VMEM((PAD * PITCH, LANES), F32),
            pltpu.VMEM((ROWS, LANES), BF16),
            pltpu.VMEM((PEERS, QUARTER, LANES), BF16),
            pltpu.VMEM((PEERS, QUARTER, LANES), BF16),
            pltpu.VMEM((PAD * AGGS, PAD), F32),
            pltpu.VMEM((LANES, LANES), F32),
            pltpu.VMEM((LANES, LANES), F32),
            pltpu.VMEM((SUBS - 1, LANES, LANES), F32),
            pltpu.VMEM((FACES, NB, NB, LANES), BF16),
            pltpu.VMEM((FACES + 1, NB, PAD, LANES), F32),
            pltpu.VMEM((ROWS, LANES), F32),
            pltpu.VMEM((ROWS, LANES), F32),
            pltpu.VMEM((FACES + 1, NB, PAD, LANES), BF16),
            pltpu.VMEM((FACES * SLOTS, 16, LANES), BF16),
            pltpu.VMEM((AGGS, 16, LANES), BF16),
            pltpu.VMEM((AGGS * PAD, NB * LANES), BF16),
            pltpu.VMEM((SLOTS * PAD, NB * LANES), BF16),
            pltpu.VMEM((FACES, 3 * LANES, LANES), BF16),
            pltpu.VMEM((GROUPS, PEERS * LANES, wide), BF16),
            pltpu.VMEM((ROWS, 3 * LANES), BF16),
            pltpu.VMEM((AGGS * PAD, wide), F32),
            pltpu.VMEM((SUBS * AGGS, PAD, wide), BF16),
            pltpu.VMEM((SUBS * AGGS, PAD, wide), BF16),
            pltpu.VMEM((SLOTS, PAD, wide), BF16),
            pltpu.VMEM((AGGS, SLOTS * PAD, wide), BF16),
            pltpu.VMEM((AGGS, SLOTS * PAD, wide), BF16),
            pltpu.VMEM((AGGS * PAD, wide), F32),
            pltpu.VMEM((GROUPS, SLOTS * PAD, LANES), F32),
            pltpu.VMEM((SLOTS * PAD, wide), F32),
            pltpu.VMEM((SLOTS * PAD, wide), BF16),
            pltpu.VMEM((SUBS - 1, 2 * PAD, wide), BF16),
            dma((11,)),
            dma((PEERS,)), dma((PEERS,)),
            dma((SUBS - 1,)), dma((SUBS - 1,)),
            dma((SUBS - 1,)), dma((SUBS - 1,)),
        ],
        compiler_params=pltpu.CompilerParams(
            collective_id=0, has_side_effects=True, vmem_limit_bytes=42 * 2**20
        ),
    )(*[pltpu.with_memory_space_constraint(a, pltpu.HBM) for a in arrays])


def per_device(
    diag_block, face_block, restrict1, neighbour, face_slot, agg_map,
    send_list, restrict2, coarse_nbr, agg2_map, coarse_slot,
):
    level = restrict2.transpose(0, 2, 1).reshape(NB * AGGS, NB)
    one, two = fused_call(
        restrict1, diag_block, neighbour, face_slot, agg_map.reshape(1, LANES), send_list, level,
        coarse_nbr, coarse_slot, agg2_map.reshape(1, AGGS), face_block,
    )
    one = one.reshape(SLOTS, NB, AGGS, NB).transpose(0, 1, 3, 2)
    two = two.reshape(SLOTS, NB, 2, NB).transpose(0, 1, 3, 2)
    return one, two


def solution(mesh):
    both = ("dom", "sub")
    placed = (
        P(None, None, both), P(None, None, None, both), P(None, None, both),
        P(None, both), P(None, both), P(both), P(None, both),
        P(None, None, both), P(None, both), P(both), P(None, both),
    )
    return jax.shard_map(
        per_device,
        mesh=mesh,
        in_specs=placed,
        out_specs=(P(None, None, None, both), P(None, None, None, both)),
        check_vma=False,
    )
```

```python
import jax
import jax.numpy as jnp
from jax import lax
from jax.experimental import pallas as pl
from jax.experimental.pallas import tpu as pltpu
from jax.sharding import PartitionSpec as P

NB = 30
PAD = 32
PITCH = 40
LANES = 128
FACES = 6
SLOTS = 8
HALO = 32
REACH = 3
PEERS = 6
GROUPS = 4
ROWS = NB * PAD
QUARTER = ROWS // GROUPS
AGGS = 16
SUBS = 4
F32 = jnp.float32
BF16 = jnp.bfloat16
MESH = pl.DeviceIdType.MESH
OFFSETS = tuple(r - REACH if r < REACH else r - REACH + 1 for r in range(PEERS))


def iota(shape, dim):
    return lax.broadcasted_iota(jnp.int32, shape, dim)


def dot(a, b):
    return jnp.dot(a, b, preferred_element_type=F32)


def split(x):
    high = x.astype(BF16)
    return high, (x - high.astype(F32)).astype(BF16)


def turn_maps(restrict_ref, wide_ref, turned_ref):
    wide_ref[pl.ds(NB * PITCH, 2 * PITCH), :] = jnp.zeros((2 * PITCH, LANES), F32)
    for n in range(NB):
        wide_ref[pl.ds(n * PITCH, NB), :] = restrict_ref[n].astype(F32)
    for m in range(NB):
        turned_ref[pl.ds(m * PAD, PAD), :] = wide_ref[pl.ds(m, PAD, stride=PITCH), :].astype(BF16)


def pack_message(r, turned_ref, list_ref, message_ref):
    lane_group = iota((QUARTER, LANES), 1) // HALO
    row = list_ref[pl.ds(r, 1), :]
    four = jnp.concatenate([row] * GROUPS, axis=1)
    pick = (iota((LANES, LANES), 0) == four).astype(BF16)
    chosen = dot(turned_ref[...], pick)
    packed = chosen[:QUARTER]
    for q in range(1, GROUPS):
        packed = jnp.where(lane_group == q, chosen[q * QUARTER : (q + 1) * QUARTER], packed)
    message_ref[r] = packed.astype(BF16)


def pack_level(level_ref, square_ref, pack_ref, coarse_ref):
    square_ref[...] = jnp.zeros(square_ref.shape, F32)
    square_ref[pl.ds(0, NB * AGGS), pl.ds(0, NB)] = level_ref[...]
    for low in range(GROUPS):
        pieces = [
            square_ref[pl.ds(q * GROUPS + low, PAD, stride=AGGS), :] for q in range(GROUPS)
        ]
        pack_ref[pl.ds(low * PAD, PAD), :] = jnp.concatenate(pieces, axis=1)
    coarse_ref[...] = pack_ref[...].T


def spread_maps(step, values, high_ref, low_ref):
    from_lane = iota((LANES, 2 * LANES), 0)
    to_lane = iota((LANES, 2 * LANES), 1)
    high, low = split(values)
    for q in range(GROUPS):
        spread = ((from_lane // PAD == q) & (from_lane % PAD == to_lane % PAD)).astype(BF16)
        blocks = pl.ds((step * GROUPS + q) * GROUPS, GROUPS)
        shape = (GROUPS, PAD, 2 * LANES)
        high_ref[blocks] = dot(high, spread).astype(BF16).reshape(shape)
        low_ref[blocks] = dot(low, spread).astype(BF16).reshape(shape)


def product(k, ten, part, near_ref, wide_ref, half_ref):
    block = 5
    total = [[None] * 4 for _ in range(block)]
    for m in range(NB):
        tiles = [near_ref[pl.ds(m * PAD + 8 * t, 8), :] for t in range(4)]
        for i in range(block):
            row = wide_ref[k, ten * 10 + part * block + i, pl.ds(m, 8, stride=0), :]
            for t in range(4):
                term = row * tiles[t]
                total[i][t] = term if m == 0 else total[i][t] + term
    for i in range(block):
        pair, side = divmod(part * block + i, 2)
        half_ref[k, ten * 5 + pair, :, pl.ds(side * LANES, LANES)] = jnp.concatenate(
            total[i], axis=0
        ).astype(BF16)


def kernel(
    restrict_hbm, diag_hbm, link_hbm, slot_hbm, group_hbm, list_hbm, level_hbm,
    far_hbm, place_hbm, owner_hbm, face_hbm,
    one_ref, two_ref,
    restrict_ref, diag_ref, link_ref, slot_ref, group_ref, list_ref, level_ref,
    far_ref, place_ref, owner_ref,
    tall_ref, turned_ref, message_ref, landed_ref, square_ref, pack_ref, coarse_ref, gathered_ref,
    face_ref, wide_ref, near_even, near_odd, half_ref, mask_ref, member_ref, left_ref, right_ref,
    pick_ref, unpack_ref, extended_ref, whole_ref, high_ref, low_ref, band_ref, block_high, block_low, mixed_ref,
    spot_ref, part_ref, small_ref, arrived_ref,
    load_sem, send_sem, recv_sem, map_send, map_recv, part_send, part_recv,
):
    dom, sub = lax.axis_index("dom"), lax.axis_index("sub")
    doms, subs = lax.axis_size("dom"), lax.axis_size("sub")
    loads = [
        pltpu.make_async_copy(source, target, load_sem.at[x])
        for x, (source, target) in enumerate(
            (
                (restrict_hbm, restrict_ref), (list_hbm, list_ref), (level_hbm, level_ref),
                (diag_hbm, diag_ref), (link_hbm, link_ref), (slot_hbm, slot_ref),
                (group_hbm, group_ref), (owner_hbm, owner_ref), (far_hbm, far_ref),
                (place_hbm, place_ref), (face_hbm, face_ref),
            )
        )
    ]
    for load in loads[:3]:
        load.start()
    barrier = pltpu.get_barrier_semaphore()
    for offset in OFFSETS:
        peer = lax.rem(dom + offset + doms, doms)
        pl.semaphore_signal(barrier, inc=1, device_id=(peer, sub), device_id_type=MESH)
    for step in range(1, SUBS):
        peer = lax.rem(sub + step, subs)
        pl.semaphore_signal(barrier, inc=1, device_id=(dom, peer), device_id_type=MESH)

    for load in loads[3:]:
        load.start()
    loads[0].wait()
    turn_maps(restrict_ref, tall_ref, turned_ref)
    loads[1].wait()

    halos, maps = [], []
    for r, offset in enumerate(OFFSETS):
        peer = lax.rem(dom - offset + doms, doms)
        halos.append(
            pltpu.make_async_remote_copy(
                src_ref=message_ref.at[r], dst_ref=landed_ref.at[r],
                send_sem=send_sem.at[r], recv_sem=recv_sem.at[r],
                device_id=(peer, sub), device_id_type=MESH,
            )
        )
    for step in range(1, SUBS):
        peer = lax.rem(sub + step, subs)
        maps.append(
            pltpu.make_async_remote_copy(
                src_ref=coarse_ref, dst_ref=gathered_ref.at[step - 1],
                send_sem=map_send.at[step - 1], recv_sem=map_recv.at[step - 1],
                device_id=(dom, peer), device_id_type=MESH,
            )
        )
    for r in range(PEERS):
        pack_message(r, turned_ref, list_ref, message_ref)
    pl.semaphore_wait(barrier, PEERS + SUBS - 1)
    for r in (0, 5, 1, 4, 2, 3):
        halos[r].start()
    loads[2].wait()
    pack_level(level_ref, square_ref, pack_ref, coarse_ref)

    for load in loads[3:10]:
        load.wait()
    for i in range(NB):
        wide_ref[FACES, i, pl.ds(0, NB), :] = diag_ref[i].astype(F32)
    near_odd[...] = turned_ref[...].astype(F32)

    def own_product(step, carry):
        for part in range(2):
            product(FACES, step, part, near_odd, wide_ref, half_ref)
        return carry

    lax.fori_loop(0, NB // 10, own_product, 0)
    for copy in maps:
        copy.start()

    for k in range(FACES):
        one_row = slot_ref[pl.ds(k, 1), :]
        row = jnp.broadcast_to(jnp.concatenate([one_row, one_row], axis=1), (8, 2 * LANES))
        for j in range(SLOTS):
            mask_ref[k * SLOTS + j] = jnp.where(row == j, 1.0, 0.0).astype(BF16)
    group = jnp.broadcast_to(group_ref[...], (16, LANES))
    for g in range(AGGS):
        member_ref[g] = jnp.where(group == g, 1.0, 0.0).astype(BF16)

    def mask_left(i, carry):
        column = pl.ds(pl.multiple_of(i * LANES, LANES), LANES)
        for part in range(2):
            tile = turned_ref[pl.ds(pl.multiple_of(i * PAD, PAD) + 16 * part, 16), :]
            for g in range(AGGS):
                left_ref[pl.ds(g * PAD + 16 * part, 16), column] = tile * member_ref[g]
        return carry

    lax.fori_loop(0, NB, mask_left, 0)
    loads[10].wait()

    def widen(k, carry):
        for i in range(NB):
            wide_ref[k, i, pl.ds(0, NB), :] = face_ref[k, i].astype(F32)
        return carry

    lax.fori_loop(0, FACES, widen, 0)

    band = iota((PAD, 2 * LANES), 1) // PAD
    for t in range(SLOTS):
        band_ref[t] = jnp.where(band == t, 1.0, 0.0).astype(BF16)
    lane_agg = iota((PAD, AGGS * PAD), 1) // PAD
    owner = jnp.zeros((PAD, AGGS * PAD), jnp.int32)
    for g in range(AGGS):
        owner = jnp.where(lane_agg == (g % GROUPS) * GROUPS + g // GROUPS, owner_ref[0, g], owner)
    level = jnp.concatenate([pack_ref[pl.ds(x * PAD, PAD), :] for x in range(GROUPS)], axis=1)
    for c in range(SLOTS):
        rows = pl.ds((c // 2) * 2 * PAD + c % 2, PAD, stride=2)
        picked = jnp.where(owner == c, level, 0.0)
        for x in range(GROUPS):
            spot_ref[x, rows, :] = picked[:, x * LANES : (x + 1) * LANES]
    spread_maps(0, coarse_ref[...], high_ref, low_ref)
    for copy in maps:
        copy.wait()
    for step in range(1, SUBS):
        spread_maps(step, gathered_ref[step - 1], high_ref, low_ref)

    def place_blocks(g, carry):
        for j in range(SLOTS):
            far = far_ref[j, g]
            step = lax.rem(sub - lax.div(far, AGGS) + SUBS, SUBS)
            agg = lax.rem(far, AGGS)
            index = step * AGGS + lax.rem(agg, GROUPS) * GROUPS + lax.div(agg, GROUPS)
            mask = band_ref[place_ref[j, g]]
            block_high[g, pl.ds(j * PAD, PAD), :] = high_ref[index] * mask
            block_low[g, pl.ds(j * PAD, PAD), :] = low_ref[index] * mask
        return carry

    lax.fori_loop(0, AGGS, place_blocks, 0)

    for k in range(FACES):
        pick_ref[k] = (iota((3 * LANES, LANES), 0) == link_ref[pl.ds(k, 1), :]).astype(BF16)
    source = iota((PEERS * LANES, 2 * LANES), 0)
    target = iota((PEERS * LANES, 2 * LANES), 1)
    landing = (source // LANES) * HALO + source % HALO == target
    for q in range(GROUPS):
        unpack_ref[q] = (landing & ((source % LANES) // HALO == q)).astype(BF16)
    extended_ref[:, pl.ds(0, LANES)] = turned_ref[...]
    for copy in halos:
        copy.wait()

    letters = jnp.concatenate([landed_ref[r] for r in range(PEERS)], axis=1)
    for q in range(GROUPS):
        far = dot(letters, unpack_ref[q]).astype(BF16)
        extended_ref[pl.ds(q * QUARTER, QUARTER), pl.ds(LANES, 2 * LANES)] = far
    near_even[...] = dot(extended_ref[...], pick_ref[0])

    steps = NB // 10
    for k in range(FACES):
        now, later = (near_even, near_odd) if k % 2 == 0 else (near_odd, near_even)

        def face_product(step, carry, k=k, now=now, later=later):
            if k + 1 < FACES:
                rows = pl.ds(pl.multiple_of(step * 10 * PAD, 10 * PAD), 10 * PAD)
                later[rows, :] = dot(extended_ref[rows, :], pick_ref[k + 1])
            for part in range(2):
                product(k, step, part, now, wide_ref, half_ref)
            return carry

        lax.fori_loop(0, steps, face_product, 0)

    def gather_slots(pair, carry):
        column = pl.ds(pl.multiple_of(pair * 2 * LANES, 2 * LANES), 2 * LANES)
        for part in range(4):
            span = pl.ds(8 * part, 8)
            half = [half_ref[k, pair, span, :] for k in range(FACES + 1)]
            for j in range(SLOTS):
                total = half[0] * mask_ref[j]
                for k in range(1, FACES):
                    total = total + half[k] * mask_ref[k * SLOTS + j]
                if j == 0:
                    total = total + half[FACES]
                right_ref[pl.ds(j * PAD + 8 * part, 8), column] = total
        return carry

    lax.fori_loop(0, NB // 2, gather_slots, 0)
    whole_ref[...] = lax.dot_general(
        left_ref[...], right_ref[...], (((1,), (1,)), ((), ())), preferred_element_type=F32
    )

    for g in range(AGGS):
        high, low = split(whole_ref[pl.ds(g * PAD, PAD), :])
        both = dot(jnp.concatenate([high, low], axis=0), block_high[g])
        rows = pl.ds(((g % GROUPS) * GROUPS + g // GROUPS) * PAD, PAD)
        mixed_ref[rows, :] = both[:PAD] + both[PAD:] + dot(high, block_low[g])
    left_high, left_low = split(jnp.concatenate([spot_ref[x] for x in range(GROUPS)], axis=1))
    right_high, right_low = split(mixed_ref[...])
    part = dot(left_high, right_high) + (dot(left_low, right_high) + dot(left_high, right_low))
    part_ref[...] = part
    small_ref[...] = part.astype(BF16)

    def lay_out(aggs):
        for g in aggs:
            for j in range(SLOTS):
                one_ref[j, pl.ds(g, NB, stride=AGGS), :] = whole_ref[
                    pl.ds(g * PAD, NB), pl.ds(j * PAD, NB)
                ]

    lay_out(range(4))
    rows = 2 * PAD
    parts = []
    for step in range(1, SUBS):
        peer = lax.rem(sub + step, subs)
        parts.append(
            pltpu.make_async_remote_copy(
                src_ref=small_ref.at[pl.ds(pl.multiple_of(peer * rows, rows), rows), :],
                dst_ref=arrived_ref.at[step - 1],
                send_sem=part_send.at[step - 1], recv_sem=part_recv.at[step - 1],
                device_id=(dom, peer), device_id_type=MESH,
            )
        )
    for copy in parts:
        copy.start()
    lay_out(range(4, AGGS))
    for copy in parts:
        copy.wait()
    own = part_ref[pl.ds(pl.multiple_of(sub * rows, rows), rows), :]
    others = [arrived_ref[x].astype(F32) for x in range(SUBS - 1)]
    total = (own + others[0]) + (others[1] + others[2])
    for t in range(SLOTS):
        two_ref[pl.ds(t * 2 * NB, 2 * NB), :] = total[: 2 * NB, t * PAD : t * PAD + NB]


def fused_call(*arrays):
    vmem = pl.BlockSpec(memory_space=pltpu.VMEM)
    hbm = pl.BlockSpec(memory_space=pltpu.HBM)
    dma = pltpu.SemaphoreType.DMA
    wide = 2 * LANES
    one_shape = (SLOTS, NB * AGGS, NB)
    return pl.pallas_call(
        kernel,
        name="galerkin",
        out_shape=(
            jax.ShapeDtypeStruct(one_shape, F32),
            jax.ShapeDtypeStruct((SLOTS * 2 * NB, NB), F32),
        ),
        in_specs=[hbm] * 11,
        out_specs=(vmem, vmem),
        scratch_shapes=[
            pltpu.VMEM((NB, NB, LANES), BF16),
            pltpu.VMEM((NB, NB, LANES), BF16),
            pltpu.VMEM((FACES, LANES), jnp.int32),
            pltpu.VMEM((FACES, LANES), jnp.int32),
            pltpu.VMEM((1, LANES), jnp.int32),
            pltpu.VMEM((PEERS, HALO), jnp.int32),
            pltpu.VMEM((NB * AGGS, NB), F32),
            pltpu.SMEM((SLOTS, AGGS), jnp.int32),
            pltpu.SMEM((SLOTS, AGGS), jnp.int32),
            pltpu.SMEM((1, AGGS), jnp.int32),
            pltpu.VMEM((PAD * PITCH, LANES), F32),
            pltpu.VMEM((ROWS, LANES), BF16),
            pltpu.VMEM((PEERS, QUARTER, LANES), BF16),
            pltpu.VMEM((PEERS, QUARTER, LANES), BF16),
            pltpu.VMEM((PAD * AGGS, PAD), F32),
            pltpu.VMEM((LANES, LANES), F32),
            pltpu.VMEM((LANES, LANES), F32),
            pltpu.VMEM((SUBS - 1, LANES, LANES), F32),
            pltpu.VMEM((FACES, NB, NB, LANES), BF16),
            pltpu.VMEM((FACES + 1, NB, PAD, LANES), F32),
            pltpu.VMEM((ROWS, LANES), F32),
            pltpu.VMEM((ROWS, LANES), F32),
            pltpu.VMEM((FACES + 1, NB // 2, PAD, wide), BF16),
            pltpu.VMEM((FACES * SLOTS, 8, wide), BF16),
            pltpu.VMEM((AGGS, 16, LANES), BF16),
            pltpu.VMEM((AGGS * PAD, NB * LANES), BF16),
            pltpu.VMEM((SLOTS * PAD, NB * LANES), BF16),
            pltpu.VMEM((FACES, 3 * LANES, LANES), BF16),
            pltpu.VMEM((GROUPS, PEERS * LANES, wide), BF16),
            pltpu.VMEM((ROWS, 3 * LANES), BF16),
            pltpu.VMEM((AGGS * PAD, wide), F32),
            pltpu.VMEM((SUBS * AGGS, PAD, wide), BF16),
            pltpu.VMEM((SUBS * AGGS, PAD, wide), BF16),
            pltpu.VMEM((SLOTS, PAD, wide), BF16),
            pltpu.VMEM((AGGS, SLOTS * PAD, wide), BF16),
            pltpu.VMEM((AGGS, SLOTS * PAD, wide), BF16),
            pltpu.VMEM((AGGS * PAD, wide), F32),
            pltpu.VMEM((GROUPS, SLOTS * PAD, LANES), F32),
            pltpu.VMEM((SLOTS * PAD, wide), F32),
            pltpu.VMEM((SLOTS * PAD, wide), BF16),
            pltpu.VMEM((SUBS - 1, 2 * PAD, wide), BF16),
            dma((11,)),
            dma((PEERS,)), dma((PEERS,)),
            dma((SUBS - 1,)), dma((SUBS - 1,)),
            dma((SUBS - 1,)), dma((SUBS - 1,)),
        ],
        compiler_params=pltpu.CompilerParams(
            collective_id=0, has_side_effects=True, vmem_limit_bytes=42 * 2**20
        ),
    )(*[pltpu.with_memory_space_constraint(a, pltpu.HBM) for a in arrays])


def per_device(
    diag_block, face_block, restrict1, neighbour, face_slot, agg_map,
    send_list, restrict2, coarse_nbr, agg2_map, coarse_slot,
):
    level = restrict2.transpose(0, 2, 1).reshape(NB * AGGS, NB)
    one, two = fused_call(
        restrict1, diag_block, neighbour, face_slot, agg_map.reshape(1, LANES), send_list, level,
        coarse_nbr, coarse_slot, agg2_map.reshape(1, AGGS), face_block,
    )
    one = one.reshape(SLOTS, NB, AGGS, NB).transpose(0, 1, 3, 2)
    two = two.reshape(SLOTS, NB, 2, NB).transpose(0, 1, 3, 2)
    return one, two


def solution(mesh):
    both = ("dom", "sub")
    placed = (
        P(None, None, both), P(None, None, None, both), P(None, None, both),
        P(None, both), P(None, both), P(both), P(None, both),
        P(None, None, both), P(None, both), P(both), P(None, both),
    )
    return jax.shard_map(
        per_device,
        mesh=mesh,
        in_specs=placed,
        out_specs=(P(None, None, None, both), P(None, None, None, both)),
        check_vma=False,
    )
```

```python
import jax
import jax.numpy as jnp
from jax import lax
from jax.experimental import pallas as pl
from jax.experimental.pallas import tpu as pltpu
from jax.sharding import PartitionSpec as P

NB = 30
PAD = 32
PITCH = 40
LANES = 128
FACES = 6
SLOTS = 8
HALO = 32
REACH = 3
PEERS = 6
GROUPS = 4
ROWS = NB * PAD
QUARTER = ROWS // GROUPS
AGGS = 16
SUBS = 4
F32 = jnp.float32
BF16 = jnp.bfloat16
MESH = pl.DeviceIdType.MESH
OFFSETS = tuple(r - REACH if r < REACH else r - REACH + 1 for r in range(PEERS))


def iota(shape, dim):
    return lax.broadcasted_iota(jnp.int32, shape, dim)


def dot(a, b):
    return jnp.dot(a, b, preferred_element_type=F32)


def split(x):
    high = x.astype(BF16)
    return high, (x - high.astype(F32)).astype(BF16)


def turn_maps(restrict_ref, wide_ref, turned_ref):
    wide_ref[pl.ds(NB * PITCH, 2 * PITCH), :] = jnp.zeros((2 * PITCH, LANES), F32)
    for n in range(NB):
        wide_ref[pl.ds(n * PITCH, NB), :] = restrict_ref[n].astype(F32)
    for m in range(NB):
        turned_ref[pl.ds(m * PAD, PAD), :] = wide_ref[pl.ds(m, PAD, stride=PITCH), :].astype(BF16)


def pack_message(r, turned_ref, list_ref, message_ref):
    lane_group = iota((QUARTER, LANES), 1) // HALO
    row = list_ref[pl.ds(r, 1), :]
    four = jnp.concatenate([row] * GROUPS, axis=1)
    pick = (iota((LANES, LANES), 0) == four).astype(BF16)
    chosen = dot(turned_ref[...], pick)
    packed = chosen[:QUARTER]
    for q in range(1, GROUPS):
        packed = jnp.where(lane_group == q, chosen[q * QUARTER : (q + 1) * QUARTER], packed)
    message_ref[r] = packed.astype(BF16)


def pack_level(level_ref, square_ref, pack_ref, coarse_ref):
    square_ref[...] = jnp.zeros(square_ref.shape, F32)
    square_ref[pl.ds(0, NB * AGGS), pl.ds(0, NB)] = level_ref[...]
    for low in range(GROUPS):
        pieces = [
            square_ref[pl.ds(q * GROUPS + low, PAD, stride=AGGS), :] for q in range(GROUPS)
        ]
        pack_ref[pl.ds(low * PAD, PAD), :] = jnp.concatenate(pieces, axis=1)
    coarse_ref[...] = pack_ref[...].T


def spread_maps(step, values, high_ref, low_ref):
    from_lane = iota((LANES, 2 * LANES), 0)
    to_lane = iota((LANES, 2 * LANES), 1)
    high, low = split(values)
    for q in range(GROUPS):
        spread = ((from_lane // PAD == q) & (from_lane % PAD == to_lane % PAD)).astype(BF16)
        blocks = pl.ds((step * GROUPS + q) * GROUPS, GROUPS)
        shape = (GROUPS, PAD, 2 * LANES)
        high_ref[blocks] = dot(high, spread).astype(BF16).reshape(shape)
        low_ref[blocks] = dot(low, spread).astype(BF16).reshape(shape)


def product(k, ten, part, near_ref, wide_ref, half_ref):
    block = 5
    total = [[None] * 4 for _ in range(block)]
    for m in range(NB):
        tiles = [near_ref[pl.ds(m * PAD + 8 * t, 8), :] for t in range(4)]
        for i in range(block):
            row = wide_ref[k, ten * 10 + part * block + i, pl.ds(m, 8, stride=0), :]
            for t in range(4):
                term = row * tiles[t]
                total[i][t] = term if m == 0 else total[i][t] + term
    for i in range(block):
        pair, side = divmod(part * block + i, 2)
        half_ref[k, ten * 5 + pair, :, pl.ds(side * LANES, LANES)] = jnp.concatenate(
            total[i], axis=0
        ).astype(BF16)


def kernel(
    restrict_hbm, diag_hbm, link_hbm, slot_hbm, group_hbm, list_hbm, level_hbm,
    far_hbm, place_hbm, owner_hbm, face_hbm,
    one_ref, two_ref,
    restrict_ref, diag_ref, link_ref, slot_ref, group_ref, list_ref, level_ref,
    far_ref, place_ref, owner_ref,
    tall_ref, turned_ref, message_ref, landed_ref, square_ref, pack_ref, coarse_ref, gathered_ref,
    face_ref, wide_ref, near_even, near_odd, half_ref, mask_ref, member_ref, left_ref, right_ref,
    pick_ref, unpack_ref, extended_ref, whole_ref, high_ref, low_ref, band_ref, block_high, block_low, mixed_ref,
    spot_ref, part_ref, small_ref, arrived_ref,
    load_sem, send_sem, recv_sem, map_send, map_recv, part_send, part_recv,
):
    dom, sub = lax.axis_index("dom"), lax.axis_index("sub")
    doms, subs = lax.axis_size("dom"), lax.axis_size("sub")
    loads = [
        pltpu.make_async_copy(source, target, load_sem.at[x])
        for x, (source, target) in enumerate(
            (
                (restrict_hbm, restrict_ref), (list_hbm, list_ref), (level_hbm, level_ref),
                (diag_hbm, diag_ref), (link_hbm, link_ref), (slot_hbm, slot_ref),
                (group_hbm, group_ref), (owner_hbm, owner_ref), (far_hbm, far_ref),
                (place_hbm, place_ref), (face_hbm, face_ref),
            )
        )
    ]
    for load in loads[:3]:
        load.start()
    barrier = pltpu.get_barrier_semaphore()
    for offset in OFFSETS:
        peer = lax.rem(dom + offset + doms, doms)
        pl.semaphore_signal(barrier, inc=1, device_id=(peer, sub), device_id_type=MESH)
    for step in range(1, SUBS):
        peer = lax.rem(sub + step, subs)
        pl.semaphore_signal(barrier, inc=1, device_id=(dom, peer), device_id_type=MESH)

    for load in loads[3:]:
        load.start()
    loads[0].wait()
    turn_maps(restrict_ref, tall_ref, turned_ref)
    loads[1].wait()

    halos, maps = [], []
    for r, offset in enumerate(OFFSETS):
        peer = lax.rem(dom - offset + doms, doms)
        halos.append(
            pltpu.make_async_remote_copy(
                src_ref=message_ref.at[r], dst_ref=landed_ref.at[r],
                send_sem=send_sem.at[r], recv_sem=recv_sem.at[r],
                device_id=(peer, sub), device_id_type=MESH,
            )
        )
    for step in range(1, SUBS):
        peer = lax.rem(sub + step, subs)
        maps.append(
            pltpu.make_async_remote_copy(
                src_ref=coarse_ref, dst_ref=gathered_ref.at[step - 1],
                send_sem=map_send.at[step - 1], recv_sem=map_recv.at[step - 1],
                device_id=(dom, peer), device_id_type=MESH,
            )
        )
    for r in range(PEERS):
        pack_message(r, turned_ref, list_ref, message_ref)
    pl.semaphore_wait(barrier, PEERS + SUBS - 1)
    for r in (0, 5, 1, 4, 2, 3):
        halos[r].start()
    loads[2].wait()
    pack_level(level_ref, square_ref, pack_ref, coarse_ref)

    for load in loads[3:10]:
        load.wait()
    for i in range(NB):
        wide_ref[FACES, i, pl.ds(0, NB), :] = diag_ref[i].astype(F32)
    near_odd[...] = turned_ref[...].astype(F32)

    def own_product(step, carry):
        for part in range(2):
            product(FACES, step, part, near_odd, wide_ref, half_ref)
        return carry

    lax.fori_loop(0, NB // 10, own_product, 0)
    for copy in maps:
        copy.start()

    for k in range(FACES):
        one_row = slot_ref[pl.ds(k, 1), :]
        row = jnp.broadcast_to(jnp.concatenate([one_row, one_row], axis=1), (8, 2 * LANES))
        for j in range(SLOTS):
            mask_ref[k * SLOTS + j] = jnp.where(row == j, 1.0, 0.0).astype(BF16)
    group = jnp.broadcast_to(group_ref[...], (16, LANES))
    for g in range(AGGS):
        member_ref[g] = jnp.where(group == g, 1.0, 0.0).astype(BF16)

    def mask_left(i, carry):
        column = pl.ds(pl.multiple_of(i * LANES, LANES), LANES)
        for part in range(2):
            tile = turned_ref[pl.ds(pl.multiple_of(i * PAD, PAD) + 16 * part, 16), :]
            for g in range(AGGS):
                left_ref[pl.ds(g * PAD + 16 * part, 16), column] = tile * member_ref[g]
        return carry

    lax.fori_loop(0, NB, mask_left, 0)
    loads[10].wait()

    def widen(k, carry):
        for i in range(NB):
            wide_ref[k, i, pl.ds(0, NB), :] = face_ref[k, i].astype(F32)
        return carry

    lax.fori_loop(0, FACES, widen, 0)

    band = iota((PAD, 2 * LANES), 1) // PAD
    for t in range(SLOTS):
        band_ref[t] = jnp.where(band == t, 1.0, 0.0).astype(BF16)
    lane_agg = iota((PAD, AGGS * PAD), 1) // PAD
    owner = jnp.zeros((PAD, AGGS * PAD), jnp.int32)
    for g in range(AGGS):
        owner = jnp.where(lane_agg == (g % GROUPS) * GROUPS + g // GROUPS, owner_ref[0, g], owner)
    level = jnp.concatenate([pack_ref[pl.ds(x * PAD, PAD), :] for x in range(GROUPS)], axis=1)
    for c in range(SLOTS):
        rows = pl.ds((c // 2) * 2 * PAD + c % 2, PAD, stride=2)
        picked = jnp.where(owner == c, level, 0.0)
        for x in range(GROUPS):
            spot_ref[x, rows, :] = picked[:, x * LANES : (x + 1) * LANES]
    spread_maps(0, coarse_ref[...], high_ref, low_ref)
    for copy in maps:
        copy.wait()
    for step in range(1, SUBS):
        spread_maps(step, gathered_ref[step - 1], high_ref, low_ref)

    def place_blocks(g, carry):
        for j in range(SLOTS):
            far = far_ref[j, g]
            step = lax.rem(sub - lax.div(far, AGGS) + SUBS, SUBS)
            agg = lax.rem(far, AGGS)
            index = step * AGGS + lax.rem(agg, GROUPS) * GROUPS + lax.div(agg, GROUPS)
            mask = band_ref[place_ref[j, g]]
            block_high[g, pl.ds(j * PAD, PAD), :] = high_ref[index] * mask
            block_low[g, pl.ds(j * PAD, PAD), :] = low_ref[index] * mask
        return carry

    lax.fori_loop(0, AGGS, place_blocks, 0)

    for k in range(FACES):
        pick_ref[k] = (iota((3 * LANES, LANES), 0) == link_ref[pl.ds(k, 1), :]).astype(BF16)
    source = iota((PEERS * LANES, 2 * LANES), 0)
    target = iota((PEERS * LANES, 2 * LANES), 1)
    landing = (source // LANES) * HALO + source % HALO == target
    for q in range(GROUPS):
        unpack_ref[q] = (landing & ((source % LANES) // HALO == q)).astype(BF16)
    extended_ref[:, pl.ds(0, LANES)] = turned_ref[...]
    for copy in halos:
        copy.wait()

    letters = jnp.concatenate([landed_ref[r] for r in range(PEERS)], axis=1)
    for q in range(GROUPS):
        far = dot(letters, unpack_ref[q]).astype(BF16)
        extended_ref[pl.ds(q * QUARTER, QUARTER), pl.ds(LANES, 2 * LANES)] = far
    near_even[...] = dot(extended_ref[...], pick_ref[0])

    steps = NB // 10
    for k in range(FACES):
        now, later = (near_even, near_odd) if k % 2 == 0 else (near_odd, near_even)

        def face_product(step, carry, k=k, now=now, later=later):
            if k + 1 < FACES:
                rows = pl.ds(pl.multiple_of(step * 10 * PAD, 10 * PAD), 10 * PAD)
                later[rows, :] = dot(extended_ref[rows, :], pick_ref[k + 1])
            for part in range(2):
                product(k, step, part, now, wide_ref, half_ref)
            return carry

        lax.fori_loop(0, steps, face_product, 0)

    def gather_slots(pair, carry):
        column = pl.ds(pl.multiple_of(pair * 2 * LANES, 2 * LANES), 2 * LANES)
        for part in range(4):
            span = pl.ds(8 * part, 8)
            half = [half_ref[k, pair, span, :] for k in range(FACES + 1)]
            for j in range(SLOTS):
                total = half[0] * mask_ref[j]
                for k in range(1, FACES):
                    total = total + half[k] * mask_ref[k * SLOTS + j]
                if j == 0:
                    total = total + half[FACES]
                right_ref[pl.ds(j * PAD + 8 * part, 8), column] = total
        return carry

    lax.fori_loop(0, NB // 2, gather_slots, 0)
    whole_ref[...] = lax.dot_general(
        left_ref[...], right_ref[...], (((1,), (1,)), ((), ())), preferred_element_type=F32
    )

    for g in range(AGGS):
        high, low = split(whole_ref[pl.ds(g * PAD, PAD), :])
        both = dot(jnp.concatenate([high, low], axis=0), block_high[g])
        rows = pl.ds(((g % GROUPS) * GROUPS + g // GROUPS) * PAD, PAD)
        mixed_ref[rows, :] = both[:PAD] + both[PAD:] + dot(high, block_low[g])
    left_high, left_low = split(jnp.concatenate([spot_ref[x] for x in range(GROUPS)], axis=1))
    right_high, right_low = split(mixed_ref[...])
    part = dot(left_high, right_high) + (dot(left_low, right_high) + dot(left_high, right_low))
    part_ref[...] = part
    small_ref[...] = part.astype(BF16)

    def lay_out(aggs):
        for g in aggs:
            for j in range(SLOTS):
                one_ref[j, pl.ds(g, NB, stride=AGGS), :] = whole_ref[
                    pl.ds(g * PAD, NB), pl.ds(j * PAD, NB)
                ]

    lay_out(range(4))
    rows = 2 * PAD
    parts = []
    for step in range(1, SUBS):
        peer = lax.rem(sub + step, subs)
        parts.append(
            pltpu.make_async_remote_copy(
                src_ref=small_ref.at[pl.ds(pl.multiple_of(peer * rows, rows), rows), :],
                dst_ref=arrived_ref.at[step - 1],
                send_sem=part_send.at[step - 1], recv_sem=part_recv.at[step - 1],
                device_id=(dom, peer), device_id_type=MESH,
            )
        )
    for copy in parts:
        copy.start()
    lay_out(range(4, AGGS))
    for copy in parts:
        copy.wait()
    own = part_ref[pl.ds(pl.multiple_of(sub * rows, rows), rows), :]
    others = [arrived_ref[x].astype(F32) for x in range(SUBS - 1)]
    total = (own + others[0]) + (others[1] + others[2])
    for t in range(SLOTS):
        two_ref[pl.ds(t * 2 * NB, 2 * NB), :] = total[: 2 * NB, t * PAD : t * PAD + NB]


def fused_call(*arrays):
    vmem = pl.BlockSpec(memory_space=pltpu.VMEM)
    hbm = pl.BlockSpec(memory_space=pltpu.HBM)
    dma = pltpu.SemaphoreType.DMA
    wide = 2 * LANES
    one_shape = (SLOTS, NB * AGGS, NB)
    return pl.pallas_call(
        kernel,
        name="galerkin",
        out_shape=(
            jax.ShapeDtypeStruct(one_shape, F32),
            jax.ShapeDtypeStruct((SLOTS * 2 * NB, NB), F32),
        ),
        in_specs=[hbm] * 11,
        out_specs=(vmem, vmem),
        scratch_shapes=[
            pltpu.VMEM((NB, NB, LANES), BF16),
            pltpu.VMEM((NB, NB, LANES), BF16),
            pltpu.VMEM((FACES, LANES), jnp.int32),
            pltpu.VMEM((FACES, LANES), jnp.int32),
            pltpu.VMEM((1, LANES), jnp.int32),
            pltpu.VMEM((PEERS, HALO), jnp.int32),
            pltpu.VMEM((NB * AGGS, NB), F32),
            pltpu.SMEM((SLOTS, AGGS), jnp.int32),
            pltpu.SMEM((SLOTS, AGGS), jnp.int32),
            pltpu.SMEM((1, AGGS), jnp.int32),
            pltpu.VMEM((PAD * PITCH, LANES), F32),
            pltpu.VMEM((ROWS, LANES), BF16),
            pltpu.VMEM((PEERS, QUARTER, LANES), BF16),
            pltpu.VMEM((PEERS, QUARTER, LANES), BF16),
            pltpu.VMEM((PAD * AGGS, PAD), F32),
            pltpu.VMEM((LANES, LANES), F32),
            pltpu.VMEM((LANES, LANES), F32),
            pltpu.VMEM((SUBS - 1, LANES, LANES), F32),
            pltpu.VMEM((FACES, NB, NB, LANES), BF16),
            pltpu.VMEM((FACES + 1, NB, PAD, LANES), F32),
            pltpu.VMEM((ROWS, LANES), F32),
            pltpu.VMEM((ROWS, LANES), F32),
            pltpu.VMEM((FACES + 1, NB // 2, PAD, wide), BF16),
            pltpu.VMEM((FACES * SLOTS, 8, wide), BF16),
            pltpu.VMEM((AGGS, 16, LANES), BF16),
            pltpu.VMEM((AGGS * PAD, NB * LANES), BF16),
            pltpu.VMEM((SLOTS * PAD, NB * LANES), BF16),
            pltpu.VMEM((FACES, 3 * LANES, LANES), BF16),
            pltpu.VMEM((GROUPS, PEERS * LANES, wide), BF16),
            pltpu.VMEM((ROWS, 3 * LANES), BF16),
            pltpu.VMEM((AGGS * PAD, wide), F32),
            pltpu.VMEM((SUBS * AGGS, PAD, wide), BF16),
            pltpu.VMEM((SUBS * AGGS, PAD, wide), BF16),
            pltpu.VMEM((SLOTS, PAD, wide), BF16),
            pltpu.VMEM((AGGS, SLOTS * PAD, wide), BF16),
            pltpu.VMEM((AGGS, SLOTS * PAD, wide), BF16),
            pltpu.VMEM((AGGS * PAD, wide), F32),
            pltpu.VMEM((GROUPS, SLOTS * PAD, LANES), F32),
            pltpu.VMEM((SLOTS * PAD, wide), F32),
            pltpu.VMEM((SLOTS * PAD, wide), BF16),
            pltpu.VMEM((SUBS - 1, 2 * PAD, wide), BF16),
            dma((11,)),
            dma((PEERS,)), dma((PEERS,)),
            dma((SUBS - 1,)), dma((SUBS - 1,)),
            dma((SUBS - 1,)), dma((SUBS - 1,)),
        ],
        compiler_params=pltpu.CompilerParams(
            collective_id=0, has_side_effects=True, vmem_limit_bytes=42 * 2**20
        ),
    )(*[pltpu.with_memory_space_constraint(a, pltpu.HBM) for a in arrays])


def place_kernel(one_ref, two_ref, one_hbm, two_hbm, sem):
    copies = [pltpu.make_async_copy(two_ref, two_hbm, sem.at[SLOTS])]
    for j in range(SLOTS):
        copies.append(pltpu.make_async_copy(one_ref.at[j], one_hbm.at[j], sem.at[j]))
    for copy in copies:
        copy.start()
    for copy in copies:
        copy.wait()


def place_call(one, two):
    anywhere = pl.BlockSpec(memory_space=pl.ANY)
    return pl.pallas_call(
        place_kernel,
        name="place",
        out_shape=(
            jax.ShapeDtypeStruct(one.shape, F32),
            jax.ShapeDtypeStruct(two.shape, F32),
        ),
        in_specs=[anywhere] * 2,
        out_specs=(anywhere,) * 2,
        scratch_shapes=[pltpu.SemaphoreType.DMA((SLOTS + 1,))],
        compiler_params=pltpu.CompilerParams(vmem_limit_bytes=2**20),
    )(one, two)


def per_device(
    diag_block, face_block, restrict1, neighbour, face_slot, agg_map,
    send_list, restrict2, coarse_nbr, agg2_map, coarse_slot,
):
    level = restrict2.transpose(0, 2, 1).reshape(NB * AGGS, NB)
    one, two = fused_call(
        restrict1, diag_block, neighbour, face_slot, agg_map.reshape(1, LANES), send_list, level,
        coarse_nbr, coarse_slot, agg2_map.reshape(1, AGGS), face_block,
    )
    one, two = place_call(one, two)
    one = one.reshape(SLOTS, NB, AGGS, NB).transpose(0, 1, 3, 2)
    two = two.reshape(SLOTS, NB, 2, NB).transpose(0, 1, 3, 2)
    return one, two


def solution(mesh):
    both = ("dom", "sub")
    placed = (
        P(None, None, both), P(None, None, None, both), P(None, None, both),
        P(None, both), P(None, both), P(both), P(None, both),
        P(None, None, both), P(None, both), P(both), P(None, both),
    )
    return jax.shard_map(
        per_device,
        mesh=mesh,
        in_specs=placed,
        out_specs=(P(None, None, None, both), P(None, None, None, both)),
        check_vma=False,
    )
```

```python
import jax
import jax.numpy as jnp
from jax import lax
from jax.experimental import pallas as pl
from jax.experimental.pallas import tpu as pltpu
from jax.sharding import PartitionSpec as P

NB = 30
PAD = 32
PITCH = 40
LANES = 128
FACES = 6
SLOTS = 8
HALO = 32
REACH = 3
PEERS = 6
GROUPS = 4
ROWS = NB * PAD
QUARTER = ROWS // GROUPS
AGGS = 16
SUBS = 4
F32 = jnp.float32
BF16 = jnp.bfloat16
MESH = pl.DeviceIdType.MESH
OFFSETS = tuple(r - REACH if r < REACH else r - REACH + 1 for r in range(PEERS))


def iota(shape, dim):
    return lax.broadcasted_iota(jnp.int32, shape, dim)


def dot(a, b):
    return jnp.dot(a, b, preferred_element_type=F32)


def split(x):
    high = x.astype(BF16)
    return high, (x - high.astype(F32)).astype(BF16)


def turn_maps(restrict_ref, wide_ref, turned_ref):
    wide_ref[pl.ds(NB * PITCH, 2 * PITCH), :] = jnp.zeros((2 * PITCH, LANES), F32)
    for n in range(NB):
        wide_ref[pl.ds(n * PITCH, NB), :] = restrict_ref[n].astype(F32)
    for m in range(NB):
        turned_ref[pl.ds(m * PAD, PAD), :] = wide_ref[pl.ds(m, PAD, stride=PITCH), :].astype(BF16)


def pack_messages(turned_ref, list_ref, message_ref):
    groups = jnp.concatenate(
        [turned_ref[pl.ds(q * QUARTER, QUARTER), :] for q in range(GROUPS)], axis=1
    )
    base = (iota((1, 2 * LANES), 1) // HALO) % GROUPS * LANES
    for pair in ((0, 5), (1, 4), (2, 3)):
        rows = [list_ref[pl.ds(r, 1), :] for r in pair for _ in range(GROUPS)]
        wanted = jnp.concatenate(rows, axis=1) + base
        pick = (iota((GROUPS * LANES, 2 * LANES), 0) == wanted).astype(BF16)
        chosen = dot(groups, pick).astype(BF16)
        for x, r in enumerate(pair):
            message_ref[r] = chosen[:, x * LANES : (x + 1) * LANES]


def pack_level(level_ref, square_ref, pack_ref, coarse_ref):
    square_ref[...] = jnp.zeros(square_ref.shape, F32)
    square_ref[pl.ds(0, NB * AGGS), pl.ds(0, NB)] = level_ref[...]
    for low in range(GROUPS):
        pieces = [
            square_ref[pl.ds(q * GROUPS + low, PAD, stride=AGGS), :] for q in range(GROUPS)
        ]
        pack_ref[pl.ds(low * PAD, PAD), :] = jnp.concatenate(pieces, axis=1)
    coarse_ref[...] = pack_ref[...].T


def spread_maps(step, values, high_ref, low_ref):
    from_lane = iota((LANES, 2 * LANES), 0)
    to_lane = iota((LANES, 2 * LANES), 1)
    high, low = split(values)
    for q in range(GROUPS):
        spread = ((from_lane // PAD == q) & (from_lane % PAD == to_lane % PAD)).astype(BF16)
        blocks = pl.ds((step * GROUPS + q) * GROUPS, GROUPS)
        shape = (GROUPS, PAD, 2 * LANES)
        high_ref[blocks] = dot(high, spread).astype(BF16).reshape(shape)
        low_ref[blocks] = dot(low, spread).astype(BF16).reshape(shape)


def product(k, ten, part, near_ref, wide_ref, half_ref):
    block = 5
    total = [[None] * 4 for _ in range(block)]
    for m in range(NB):
        tiles = [near_ref[pl.ds(m * PAD + 8 * t, 8), :] for t in range(4)]
        for i in range(block):
            row = wide_ref[k, ten * 10 + part * block + i, pl.ds(m, 8, stride=0), :]
            for t in range(4):
                term = row * tiles[t]
                total[i][t] = term if m == 0 else total[i][t] + term
    for i in range(block):
        pair, side = divmod(part * block + i, 2)
        half_ref[k, ten * 5 + pair, :, pl.ds(side * LANES, LANES)] = jnp.concatenate(
            total[i], axis=0
        ).astype(BF16)


def kernel(
    restrict_hbm, diag_hbm, link_hbm, slot_hbm, group_hbm, list_hbm, level_hbm,
    far_hbm, place_hbm, owner_hbm, face_hbm,
    one_ref, two_ref,
    restrict_ref, diag_ref, link_ref, slot_ref, group_ref, list_ref, level_ref,
    far_ref, place_ref, owner_ref,
    tall_ref, turned_ref, message_ref, landed_ref, square_ref, pack_ref, coarse_ref, gathered_ref,
    face_ref, wide_ref, near_even, near_odd, half_ref, mask_ref, member_ref, left_ref, right_ref,
    pick_ref, unpack_ref, extended_ref, whole_ref, high_ref, low_ref, band_ref, block_high, block_low, mixed_ref,
    spot_ref, part_ref, small_ref, arrived_ref,
    load_sem, send_sem, recv_sem, map_send, map_recv, part_send, part_recv,
):
    dom, sub = lax.axis_index("dom"), lax.axis_index("sub")
    doms, subs = lax.axis_size("dom"), lax.axis_size("sub")
    loads = [
        pltpu.make_async_copy(source, target, load_sem.at[x])
        for x, (source, target) in enumerate(
            (
                (restrict_hbm, restrict_ref), (list_hbm, list_ref), (level_hbm, level_ref),
                (diag_hbm, diag_ref), (link_hbm, link_ref), (slot_hbm, slot_ref),
                (group_hbm, group_ref), (owner_hbm, owner_ref), (far_hbm, far_ref),
                (place_hbm, place_ref), (face_hbm, face_ref),
            )
        )
    ]
    for load in loads[:3]:
        load.start()
    barrier = pltpu.get_barrier_semaphore()
    for offset in OFFSETS:
        peer = lax.rem(dom + offset + doms, doms)
        pl.semaphore_signal(barrier, inc=1, device_id=(peer, sub), device_id_type=MESH)
    for step in range(1, SUBS):
        peer = lax.rem(sub + step, subs)
        pl.semaphore_signal(barrier, inc=1, device_id=(dom, peer), device_id_type=MESH)

    for load in loads[3:]:
        load.start()
    loads[0].wait()
    turn_maps(restrict_ref, tall_ref, turned_ref)
    loads[1].wait()

    halos, maps = [], []
    for r, offset in enumerate(OFFSETS):
        peer = lax.rem(dom - offset + doms, doms)
        halos.append(
            pltpu.make_async_remote_copy(
                src_ref=message_ref.at[r], dst_ref=landed_ref.at[r],
                send_sem=send_sem.at[r], recv_sem=recv_sem.at[r],
                device_id=(peer, sub), device_id_type=MESH,
            )
        )
    for step in range(1, SUBS):
        peer = lax.rem(sub + step, subs)
        maps.append(
            pltpu.make_async_remote_copy(
                src_ref=coarse_ref, dst_ref=gathered_ref.at[step - 1],
                send_sem=map_send.at[step - 1], recv_sem=map_recv.at[step - 1],
                device_id=(dom, peer), device_id_type=MESH,
            )
        )
    pack_messages(turned_ref, list_ref, message_ref)
    pl.semaphore_wait(barrier, PEERS + SUBS - 1)
    for r in (0, 5, 1, 4, 2, 3):
        halos[r].start()
    loads[2].wait()
    pack_level(level_ref, square_ref, pack_ref, coarse_ref)

    for load in loads[3:10]:
        load.wait()
    for i in range(NB):
        wide_ref[FACES, i, pl.ds(0, NB), :] = diag_ref[i].astype(F32)
    near_odd[...] = turned_ref[...].astype(F32)

    def own_product(step, carry):
        for part in range(2):
            product(FACES, step, part, near_odd, wide_ref, half_ref)
        return carry

    lax.fori_loop(0, NB // 10, own_product, 0)
    for copy in maps:
        copy.start()

    for k in range(FACES):
        one_row = slot_ref[pl.ds(k, 1), :]
        row = jnp.broadcast_to(jnp.concatenate([one_row, one_row], axis=1), (8, 2 * LANES))
        for j in range(SLOTS):
            mask_ref[k * SLOTS + j] = jnp.where(row == j, 1.0, 0.0).astype(BF16)
    group = jnp.broadcast_to(group_ref[...], (16, LANES))
    for g in range(AGGS):
        member_ref[g] = jnp.where(group == g, 1.0, 0.0).astype(BF16)

    def mask_left(i, carry):
        column = pl.ds(pl.multiple_of(i * LANES, LANES), LANES)
        for part in range(2):
            tile = turned_ref[pl.ds(pl.multiple_of(i * PAD, PAD) + 16 * part, 16), :]
            for g in range(AGGS):
                left_ref[pl.ds(g * PAD + 16 * part, 16), column] = tile * member_ref[g]
        return carry

    lax.fori_loop(0, NB, mask_left, 0)
    loads[10].wait()

    def widen(k, carry):
        for i in range(NB):
            wide_ref[k, i, pl.ds(0, NB), :] = face_ref[k, i].astype(F32)
        return carry

    lax.fori_loop(0, FACES, widen, 0)

    band = iota((PAD, 2 * LANES), 1) // PAD
    for t in range(SLOTS):
        band_ref[t] = jnp.where(band == t, 1.0, 0.0).astype(BF16)
    lane_agg = iota((PAD, AGGS * PAD), 1) // PAD
    owner = jnp.zeros((PAD, AGGS * PAD), jnp.int32)
    for g in range(AGGS):
        owner = jnp.where(lane_agg == (g % GROUPS) * GROUPS + g // GROUPS, owner_ref[0, g], owner)
    level = jnp.concatenate([pack_ref[pl.ds(x * PAD, PAD), :] for x in range(GROUPS)], axis=1)
    for c in range(SLOTS):
        rows = pl.ds((c // 2) * 2 * PAD + c % 2, PAD, stride=2)
        picked = jnp.where(owner == c, level, 0.0)
        for x in range(GROUPS):
            spot_ref[x, rows, :] = picked[:, x * LANES : (x + 1) * LANES]
    spread_maps(0, coarse_ref[...], high_ref, low_ref)
    for copy in maps:
        copy.wait()
    for step in range(1, SUBS):
        spread_maps(step, gathered_ref[step - 1], high_ref, low_ref)

    def place_blocks(g, carry):
        for j in range(SLOTS):
            far = far_ref[j, g]
            step = lax.rem(sub - lax.div(far, AGGS) + SUBS, SUBS)
            agg = lax.rem(far, AGGS)
            index = step * AGGS + lax.rem(agg, GROUPS) * GROUPS + lax.div(agg, GROUPS)
            mask = band_ref[place_ref[j, g]]
            block_high[g, pl.ds(j * PAD, PAD), :] = high_ref[index] * mask
            block_low[g, pl.ds(j * PAD, PAD), :] = low_ref[index] * mask
        return carry

    lax.fori_loop(0, AGGS, place_blocks, 0)

    for k in range(FACES):
        pick_ref[k] = (iota((3 * LANES, LANES), 0) == link_ref[pl.ds(k, 1), :]).astype(BF16)
    source = iota((PEERS * LANES, 2 * LANES), 0)
    target = iota((PEERS * LANES, 2 * LANES), 1)
    landing = (source // LANES) * HALO + source % HALO == target
    for q in range(GROUPS):
        unpack_ref[q] = (landing & ((source % LANES) // HALO == q)).astype(BF16)
    extended_ref[:, pl.ds(0, LANES)] = turned_ref[...]
    for copy in halos:
        copy.wait()

    letters = jnp.concatenate([landed_ref[r] for r in range(PEERS)], axis=1)
    for q in range(GROUPS):
        far = dot(letters, unpack_ref[q]).astype(BF16)
        extended_ref[pl.ds(q * QUARTER, QUARTER), pl.ds(LANES, 2 * LANES)] = far
    near_even[...] = dot(extended_ref[...], pick_ref[0])

    steps = NB // 10
    for k in range(FACES):
        now, later = (near_even, near_odd) if k % 2 == 0 else (near_odd, near_even)

        def face_product(step, carry, k=k, now=now, later=later):
            if k + 1 < FACES:
                rows = pl.ds(pl.multiple_of(step * 10 * PAD, 10 * PAD), 10 * PAD)
                later[rows, :] = dot(extended_ref[rows, :], pick_ref[k + 1])
            for part in range(2):
                product(k, step, part, now, wide_ref, half_ref)
            return carry

        lax.fori_loop(0, steps, face_product, 0)

    def gather_slots(pair, carry):
        column = pl.ds(pl.multiple_of(pair * 2 * LANES, 2 * LANES), 2 * LANES)
        for part in range(4):
            span = pl.ds(8 * part, 8)
            half = [half_ref[k, pair, span, :] for k in range(FACES + 1)]
            for j in range(SLOTS):
                total = half[0] * mask_ref[j]
                for k in range(1, FACES):
                    total = total + half[k] * mask_ref[k * SLOTS + j]
                if j == 0:
                    total = total + half[FACES]
                right_ref[pl.ds(j * PAD + 8 * part, 8), column] = total
        return carry

    lax.fori_loop(0, NB // 2, gather_slots, 0)
    whole_ref[...] = lax.dot_general(
        left_ref[...], right_ref[...], (((1,), (1,)), ((), ())), preferred_element_type=F32
    )

    for g in range(AGGS):
        high, low = split(whole_ref[pl.ds(g * PAD, PAD), :])
        both = dot(jnp.concatenate([high, low], axis=0), block_high[g])
        rows = pl.ds(((g % GROUPS) * GROUPS + g // GROUPS) * PAD, PAD)
        mixed_ref[rows, :] = both[:PAD] + both[PAD:] + dot(high, block_low[g])
    left_high, left_low = split(jnp.concatenate([spot_ref[x] for x in range(GROUPS)], axis=1))
    right_high, right_low = split(mixed_ref[...])
    part = dot(left_high, right_high) + (dot(left_low, right_high) + dot(left_high, right_low))
    part_ref[...] = part
    small_ref[...] = part.astype(BF16)

    def lay_out(aggs):
        for g in aggs:
            for j in range(SLOTS):
                one_ref[j, pl.ds(g, NB, stride=AGGS), :] = whole_ref[
                    pl.ds(g * PAD, NB), pl.ds(j * PAD, NB)
                ]

    lay_out(range(4))
    rows = 2 * PAD
    parts = []
    for step in range(1, SUBS):
        peer = lax.rem(sub + step, subs)
        parts.append(
            pltpu.make_async_remote_copy(
                src_ref=small_ref.at[pl.ds(pl.multiple_of(peer * rows, rows), rows), :],
                dst_ref=arrived_ref.at[step - 1],
                send_sem=part_send.at[step - 1], recv_sem=part_recv.at[step - 1],
                device_id=(dom, peer), device_id_type=MESH,
            )
        )
    for step in (2, 1, 3):
        parts[step - 1].start()
    lay_out(range(4, AGGS))
    for copy in parts:
        copy.wait()
    own = part_ref[pl.ds(pl.multiple_of(sub * rows, rows), rows), :]
    others = [arrived_ref[x].astype(F32) for x in range(SUBS - 1)]
    total = (own + others[0]) + (others[1] + others[2])
    for t in range(SLOTS):
        two_ref[pl.ds(t * 2 * NB, 2 * NB), :] = total[: 2 * NB, t * PAD : t * PAD + NB]


def fused_call(*arrays):
    vmem = pl.BlockSpec(memory_space=pltpu.VMEM)
    hbm = pl.BlockSpec(memory_space=pltpu.HBM)
    dma = pltpu.SemaphoreType.DMA
    wide = 2 * LANES
    one_shape = (SLOTS, NB * AGGS, NB)
    return pl.pallas_call(
        kernel,
        name="galerkin",
        out_shape=(
            jax.ShapeDtypeStruct(one_shape, F32),
            jax.ShapeDtypeStruct((SLOTS * 2 * NB, NB), F32),
        ),
        in_specs=[hbm] * 11,
        out_specs=(vmem, vmem),
        scratch_shapes=[
            pltpu.VMEM((NB, NB, LANES), BF16),
            pltpu.VMEM((NB, NB, LANES), BF16),
            pltpu.VMEM((FACES, LANES), jnp.int32),
            pltpu.VMEM((FACES, LANES), jnp.int32),
            pltpu.VMEM((1, LANES), jnp.int32),
            pltpu.VMEM((PEERS, HALO), jnp.int32),
            pltpu.VMEM((NB * AGGS, NB), F32),
            pltpu.SMEM((SLOTS, AGGS), jnp.int32),
            pltpu.SMEM((SLOTS, AGGS), jnp.int32),
            pltpu.SMEM((1, AGGS), jnp.int32),
            pltpu.VMEM((PAD * PITCH, LANES), F32),
            pltpu.VMEM((ROWS, LANES), BF16),
            pltpu.VMEM((PEERS, QUARTER, LANES), BF16),
            pltpu.VMEM((PEERS, QUARTER, LANES), BF16),
            pltpu.VMEM((PAD * AGGS, PAD), F32),
            pltpu.VMEM((LANES, LANES), F32),
            pltpu.VMEM((LANES, LANES), F32),
            pltpu.VMEM((SUBS - 1, LANES, LANES), F32),
            pltpu.VMEM((FACES, NB, NB, LANES), BF16),
            pltpu.VMEM((FACES + 1, NB, PAD, LANES), F32),
            pltpu.VMEM((ROWS, LANES), F32),
            pltpu.VMEM((ROWS, LANES), F32),
            pltpu.VMEM((FACES + 1, NB // 2, PAD, wide), BF16),
            pltpu.VMEM((FACES * SLOTS, 8, wide), BF16),
            pltpu.VMEM((AGGS, 16, LANES), BF16),
            pltpu.VMEM((AGGS * PAD, NB * LANES), BF16),
            pltpu.VMEM((SLOTS * PAD, NB * LANES), BF16),
            pltpu.VMEM((FACES, 3 * LANES, LANES), BF16),
            pltpu.VMEM((GROUPS, PEERS * LANES, wide), BF16),
            pltpu.VMEM((ROWS, 3 * LANES), BF16),
            pltpu.VMEM((AGGS * PAD, wide), F32),
            pltpu.VMEM((SUBS * AGGS, PAD, wide), BF16),
            pltpu.VMEM((SUBS * AGGS, PAD, wide), BF16),
            pltpu.VMEM((SLOTS, PAD, wide), BF16),
            pltpu.VMEM((AGGS, SLOTS * PAD, wide), BF16),
            pltpu.VMEM((AGGS, SLOTS * PAD, wide), BF16),
            pltpu.VMEM((AGGS * PAD, wide), F32),
            pltpu.VMEM((GROUPS, SLOTS * PAD, LANES), F32),
            pltpu.VMEM((SLOTS * PAD, wide), F32),
            pltpu.VMEM((SLOTS * PAD, wide), BF16),
            pltpu.VMEM((SUBS - 1, 2 * PAD, wide), BF16),
            dma((11,)),
            dma((PEERS,)), dma((PEERS,)),
            dma((SUBS - 1,)), dma((SUBS - 1,)),
            dma((SUBS - 1,)), dma((SUBS - 1,)),
        ],
        compiler_params=pltpu.CompilerParams(
            collective_id=0, has_side_effects=True, vmem_limit_bytes=42 * 2**20
        ),
    )(*[pltpu.with_memory_space_constraint(a, pltpu.HBM) for a in arrays])


def place_kernel(one_ref, two_ref, one_hbm, two_hbm, sem):
    copies = [pltpu.make_async_copy(two_ref, two_hbm, sem.at[SLOTS])]
    for j in range(SLOTS):
        copies.append(pltpu.make_async_copy(one_ref.at[j], one_hbm.at[j], sem.at[j]))
    for copy in copies:
        copy.start()
    for copy in copies:
        copy.wait()


def place_call(one, two):
    anywhere = pl.BlockSpec(memory_space=pl.ANY)
    return pl.pallas_call(
        place_kernel,
        name="place",
        out_shape=(
            jax.ShapeDtypeStruct(one.shape, F32),
            jax.ShapeDtypeStruct(two.shape, F32),
        ),
        in_specs=[anywhere] * 2,
        out_specs=(anywhere,) * 2,
        scratch_shapes=[pltpu.SemaphoreType.DMA((SLOTS + 1,))],
        compiler_params=pltpu.CompilerParams(vmem_limit_bytes=2**20),
    )(one, two)


def per_device(
    diag_block, face_block, restrict1, neighbour, face_slot, agg_map,
    send_list, restrict2, coarse_nbr, agg2_map, coarse_slot,
):
    level = restrict2.transpose(0, 2, 1).reshape(NB * AGGS, NB)
    one, two = fused_call(
        restrict1, diag_block, neighbour, face_slot, agg_map.reshape(1, LANES), send_list, level,
        coarse_nbr, coarse_slot, agg2_map.reshape(1, AGGS), face_block,
    )
    one, two = place_call(one, two)
    one = one.reshape(SLOTS, NB, AGGS, NB).transpose(0, 1, 3, 2)
    two = two.reshape(SLOTS, NB, 2, NB).transpose(0, 1, 3, 2)
    return one, two


def solution(mesh):
    both = ("dom", "sub")
    placed = (
        P(None, None, both), P(None, None, None, both), P(None, None, both),
        P(None, both), P(None, both), P(both), P(None, both),
        P(None, None, both), P(None, both), P(both), P(None, both),
    )
    return jax.shard_map(
        per_device,
        mesh=mesh,
        in_specs=placed,
        out_specs=(P(None, None, None, both), P(None, None, None, both)),
        check_vma=False,
    )
```

```python
import jax
import jax.numpy as jnp
from jax import lax
from jax.experimental import pallas as pl
from jax.experimental.pallas import tpu as pltpu
from jax.sharding import PartitionSpec as P

NB = 30
PAD = 32
PITCH = 40
LANES = 128
FACES = 6
SLOTS = 8
HALO = 32
REACH = 3
PEERS = 6
GROUPS = 4
ROWS = NB * PAD
QUARTER = ROWS // GROUPS
AGGS = 16
SUBS = 4
F32 = jnp.float32
BF16 = jnp.bfloat16
MESH = pl.DeviceIdType.MESH
OFFSETS = tuple(r - REACH if r < REACH else r - REACH + 1 for r in range(PEERS))


def iota(shape, dim):
    return lax.broadcasted_iota(jnp.int32, shape, dim)


def dot(a, b):
    return jnp.dot(a, b, preferred_element_type=F32)


def split(x):
    high = x.astype(BF16)
    return high, (x - high.astype(F32)).astype(BF16)


def turn_maps(restrict_ref, wide_ref, turned_ref):
    wide_ref[pl.ds(NB * PITCH, 2 * PITCH), :] = jnp.zeros((2 * PITCH, LANES), F32)
    for n in range(NB):
        wide_ref[pl.ds(n * PITCH, NB), :] = restrict_ref[n].astype(F32)
    for m in range(NB):
        turned_ref[pl.ds(m * PAD, PAD), :] = wide_ref[pl.ds(m, PAD, stride=PITCH), :].astype(BF16)


def pack_messages(turned_ref, list_ref, message_ref):
    groups = jnp.concatenate(
        [turned_ref[pl.ds(q * QUARTER, QUARTER), :] for q in range(GROUPS)], axis=1
    )
    base = (iota((1, 2 * LANES), 1) // HALO) % GROUPS * LANES
    for pair in ((0, 5), (1, 4), (2, 3)):
        rows = [list_ref[pl.ds(r, 1), :] for r in pair for _ in range(GROUPS)]
        wanted = jnp.concatenate(rows, axis=1) + base
        pick = (iota((GROUPS * LANES, 2 * LANES), 0) == wanted).astype(BF16)
        chosen = dot(groups, pick).astype(BF16)
        for x, r in enumerate(pair):
            message_ref[r] = chosen[:, x * LANES : (x + 1) * LANES]


def pack_level(level_ref, square_ref, pack_ref, coarse_ref):
    square_ref[...] = jnp.zeros(square_ref.shape, F32)
    square_ref[pl.ds(0, NB * AGGS), pl.ds(0, NB)] = level_ref[...]
    for low in range(GROUPS):
        pieces = [
            square_ref[pl.ds(q * GROUPS + low, PAD, stride=AGGS), :] for q in range(GROUPS)
        ]
        pack_ref[pl.ds(low * PAD, PAD), :] = jnp.concatenate(pieces, axis=1)
    coarse_ref[...] = pack_ref[...].T


def spread_maps(step, values, high_ref, low_ref):
    from_lane = iota((LANES, 2 * LANES), 0)
    to_lane = iota((LANES, 2 * LANES), 1)
    high, low = split(values)
    for q in range(GROUPS):
        spread = ((from_lane // PAD == q) & (from_lane % PAD == to_lane % PAD)).astype(BF16)
        blocks = pl.ds((step * GROUPS + q) * GROUPS, GROUPS)
        shape = (GROUPS, PAD, 2 * LANES)
        high_ref[blocks] = dot(high, spread).astype(BF16).reshape(shape)
        low_ref[blocks] = dot(low, spread).astype(BF16).reshape(shape)


def product(k, ten, part, near_ref, wide_ref, half_ref):
    block = 5
    total = [[None] * 4 for _ in range(block)]
    for m in range(NB):
        tiles = [near_ref[pl.ds(m * PAD + 8 * t, 8), :] for t in range(4)]
        for i in range(block):
            row = wide_ref[k, ten * 10 + part * block + i, pl.ds(m, 8, stride=0), :]
            for t in range(4):
                term = row * tiles[t]
                total[i][t] = term if m == 0 else total[i][t] + term
    for i in range(block):
        pair, side = divmod(part * block + i, 2)
        half_ref[k, ten * 5 + pair, :, pl.ds(side * LANES, LANES)] = jnp.concatenate(
            total[i], axis=0
        ).astype(BF16)


def kernel(
    restrict_hbm, diag_hbm, link_hbm, slot_hbm, group_hbm, list_hbm, level_hbm,
    far_hbm, place_hbm, owner_hbm, face_hbm,
    one_ref, two_ref,
    restrict_ref, diag_ref, link_ref, slot_ref, group_ref, list_ref, level_ref,
    far_ref, place_ref, owner_ref,
    tall_ref, turned_ref, message_ref, landed_ref, square_ref, pack_ref, coarse_ref, gathered_ref,
    face_ref, wide_ref, near_even, near_odd, half_ref, mask_ref, member_ref, left_ref, right_ref,
    pick_ref, unpack_ref, extended_ref, whole_ref, high_ref, low_ref, band_ref, block_high, block_low, mixed_ref,
    spot_ref, part_ref, small_ref, arrived_ref,
    load_sem, send_sem, recv_sem, map_send, map_recv, part_send, part_recv,
):
    dom, sub = lax.axis_index("dom"), lax.axis_index("sub")
    doms, subs = lax.axis_size("dom"), lax.axis_size("sub")
    loads = [
        pltpu.make_async_copy(source, target, load_sem.at[x])
        for x, (source, target) in enumerate(
            (
                (restrict_hbm, restrict_ref), (list_hbm, list_ref), (level_hbm, level_ref),
                (diag_hbm, diag_ref), (link_hbm, link_ref), (slot_hbm, slot_ref),
                (group_hbm, group_ref), (owner_hbm, owner_ref), (far_hbm, far_ref),
                (place_hbm, place_ref), (face_hbm, face_ref),
            )
        )
    ]
    for load in loads[:3]:
        load.start()
    barrier = pltpu.get_barrier_semaphore()
    for offset in OFFSETS:
        peer = lax.rem(dom + offset + doms, doms)
        pl.semaphore_signal(barrier, inc=1, device_id=(peer, sub), device_id_type=MESH)
    for step in range(1, SUBS):
        peer = lax.rem(sub + step, subs)
        pl.semaphore_signal(barrier, inc=1, device_id=(dom, peer), device_id_type=MESH)

    for load in loads[3:]:
        load.start()
    loads[0].wait()
    turn_maps(restrict_ref, tall_ref, turned_ref)
    loads[1].wait()

    halos, maps = [], []
    for r, offset in enumerate(OFFSETS):
        peer = lax.rem(dom - offset + doms, doms)
        halos.append(
            pltpu.make_async_remote_copy(
                src_ref=message_ref.at[r], dst_ref=landed_ref.at[r],
                send_sem=send_sem.at[r], recv_sem=recv_sem.at[r],
                device_id=(peer, sub), device_id_type=MESH,
            )
        )
    for step in range(1, SUBS):
        peer = lax.rem(sub + step, subs)
        maps.append(
            pltpu.make_async_remote_copy(
                src_ref=coarse_ref, dst_ref=gathered_ref.at[step - 1],
                send_sem=map_send.at[step - 1], recv_sem=map_recv.at[step - 1],
                device_id=(dom, peer), device_id_type=MESH,
            )
        )
    pack_messages(turned_ref, list_ref, message_ref)
    pl.semaphore_wait(barrier, PEERS + SUBS - 1)
    for r in (0, 5, 1, 4, 2, 3):
        halos[r].start()
    loads[2].wait()
    pack_level(level_ref, square_ref, pack_ref, coarse_ref)

    for load in loads[3:10]:
        load.wait()
    for i in range(NB):
        wide_ref[FACES, i, pl.ds(0, NB), :] = diag_ref[i].astype(F32)
    near_odd[...] = turned_ref[...].astype(F32)

    def own_product(step, carry):
        for part in range(2):
            product(FACES, step, part, near_odd, wide_ref, half_ref)
        return carry

    for step in (2, 1, 3):
        maps[step - 1].start()
    lax.fori_loop(0, NB // 10, own_product, 0)

    for k in range(FACES):
        one_row = slot_ref[pl.ds(k, 1), :]
        row = jnp.broadcast_to(jnp.concatenate([one_row, one_row], axis=1), (8, 2 * LANES))
        for j in range(SLOTS):
            mask_ref[k * SLOTS + j] = jnp.where(row == j, 1.0, 0.0).astype(BF16)
    group = jnp.broadcast_to(group_ref[...], (16, LANES))
    for g in range(AGGS):
        member_ref[g] = jnp.where(group == g, 1.0, 0.0).astype(BF16)

    def mask_left(i, carry):
        column = pl.ds(pl.multiple_of(i * LANES, LANES), LANES)
        for part in range(2):
            tile = turned_ref[pl.ds(pl.multiple_of(i * PAD, PAD) + 16 * part, 16), :]
            for g in range(AGGS):
                left_ref[pl.ds(g * PAD + 16 * part, 16), column] = tile * member_ref[g]
        return carry

    lax.fori_loop(0, NB, mask_left, 0)
    loads[10].wait()

    def widen(k, carry):
        for i in range(NB):
            wide_ref[k, i, pl.ds(0, NB), :] = face_ref[k, i].astype(F32)
        return carry

    lax.fori_loop(0, FACES, widen, 0)

    band = iota((PAD, 2 * LANES), 1) // PAD
    for t in range(SLOTS):
        band_ref[t] = jnp.where(band == t, 1.0, 0.0).astype(BF16)
    lane_agg = iota((PAD, AGGS * PAD), 1) // PAD
    owner = jnp.zeros((PAD, AGGS * PAD), jnp.int32)
    for g in range(AGGS):
        owner = jnp.where(lane_agg == (g % GROUPS) * GROUPS + g // GROUPS, owner_ref[0, g], owner)
    level = jnp.concatenate([pack_ref[pl.ds(x * PAD, PAD), :] for x in range(GROUPS)], axis=1)
    for c in range(SLOTS):
        rows = pl.ds((c // 2) * 2 * PAD + c % 2, PAD, stride=2)
        picked = jnp.where(owner == c, level, 0.0)
        for x in range(GROUPS):
            spot_ref[x, rows, :] = picked[:, x * LANES : (x + 1) * LANES]
    for k in range(FACES):
        pick_ref[k] = (iota((3 * LANES, LANES), 0) == link_ref[pl.ds(k, 1), :]).astype(BF16)
    source = iota((PEERS * LANES, 2 * LANES), 0)
    target = iota((PEERS * LANES, 2 * LANES), 1)
    landing = (source // LANES) * HALO + source % HALO == target
    for q in range(GROUPS):
        unpack_ref[q] = (landing & ((source % LANES) // HALO == q)).astype(BF16)
    extended_ref[:, pl.ds(0, LANES)] = turned_ref[...]
    spread_maps(0, coarse_ref[...], high_ref, low_ref)
    for copy in maps:
        copy.wait()
    for step in range(1, SUBS):
        spread_maps(step, gathered_ref[step - 1], high_ref, low_ref)

    def place_blocks(g, carry):
        for j in range(SLOTS):
            far = far_ref[j, g]
            step = lax.rem(sub - lax.div(far, AGGS) + SUBS, SUBS)
            agg = lax.rem(far, AGGS)
            index = step * AGGS + lax.rem(agg, GROUPS) * GROUPS + lax.div(agg, GROUPS)
            mask = band_ref[place_ref[j, g]]
            block_high[g, pl.ds(j * PAD, PAD), :] = high_ref[index] * mask
            block_low[g, pl.ds(j * PAD, PAD), :] = low_ref[index] * mask
        return carry

    lax.fori_loop(0, AGGS, place_blocks, 0)

    for copy in halos:
        copy.wait()

    letters = jnp.concatenate([landed_ref[r] for r in range(PEERS)], axis=1)
    for q in range(GROUPS):
        far = dot(letters, unpack_ref[q]).astype(BF16)
        extended_ref[pl.ds(q * QUARTER, QUARTER), pl.ds(LANES, 2 * LANES)] = far
    near_even[...] = dot(extended_ref[...], pick_ref[0])

    steps = NB // 10
    for k in range(FACES):
        now, later = (near_even, near_odd) if k % 2 == 0 else (near_odd, near_even)

        def face_product(step, carry, k=k, now=now, later=later):
            if k + 1 < FACES:
                rows = pl.ds(pl.multiple_of(step * 10 * PAD, 10 * PAD), 10 * PAD)
                later[rows, :] = dot(extended_ref[rows, :], pick_ref[k + 1])
            for part in range(2):
                product(k, step, part, now, wide_ref, half_ref)
            return carry

        lax.fori_loop(0, steps, face_product, 0)

    def gather_slots(pair, carry):
        column = pl.ds(pl.multiple_of(pair * 2 * LANES, 2 * LANES), 2 * LANES)
        for part in range(4):
            span = pl.ds(8 * part, 8)
            half = [half_ref[k, pair, span, :] for k in range(FACES + 1)]
            for j in range(SLOTS):
                total = half[0] * mask_ref[j]
                for k in range(1, FACES):
                    total = total + half[k] * mask_ref[k * SLOTS + j]
                if j == 0:
                    total = total + half[FACES]
                right_ref[pl.ds(j * PAD + 8 * part, 8), column] = total
        return carry

    lax.fori_loop(0, NB // 2, gather_slots, 0)
    whole_ref[...] = lax.dot_general(
        left_ref[...], right_ref[...], (((1,), (1,)), ((), ())), preferred_element_type=F32
    )

    for g in range(AGGS):
        high, low = split(whole_ref[pl.ds(g * PAD, PAD), :])
        both = dot(jnp.concatenate([high, low], axis=0), block_high[g])
        rows = pl.ds(((g % GROUPS) * GROUPS + g // GROUPS) * PAD, PAD)
        mixed_ref[rows, :] = both[:PAD] + both[PAD:] + dot(high, block_low[g])
    left_high, left_low = split(jnp.concatenate([spot_ref[x] for x in range(GROUPS)], axis=1))
    right_high, right_low = split(mixed_ref[...])
    part = dot(left_high, right_high) + (dot(left_low, right_high) + dot(left_high, right_low))
    part_ref[...] = part
    small_ref[...] = part.astype(BF16)

    def lay_out(aggs):
        for g in aggs:
            for j in range(SLOTS):
                one_ref[j, pl.ds(g, NB, stride=AGGS), :] = whole_ref[
                    pl.ds(g * PAD, NB), pl.ds(j * PAD, NB)
                ]

    lay_out(range(4))
    rows = 2 * PAD
    parts = []
    for step in range(1, SUBS):
        peer = lax.rem(sub + step, subs)
        parts.append(
            pltpu.make_async_remote_copy(
                src_ref=small_ref.at[pl.ds(pl.multiple_of(peer * rows, rows), rows), :],
                dst_ref=arrived_ref.at[step - 1],
                send_sem=part_send.at[step - 1], recv_sem=part_recv.at[step - 1],
                device_id=(dom, peer), device_id_type=MESH,
            )
        )
    for step in (2, 1, 3):
        parts[step - 1].start()
    lay_out(range(4, AGGS))
    for copy in parts:
        copy.wait()
    own = part_ref[pl.ds(pl.multiple_of(sub * rows, rows), rows), :]
    others = [arrived_ref[x].astype(F32) for x in range(SUBS - 1)]
    total = (own + others[0]) + (others[1] + others[2])
    for t in range(SLOTS):
        two_ref[pl.ds(t * 2 * NB, 2 * NB), :] = total[: 2 * NB, t * PAD : t * PAD + NB]


def fused_call(*arrays):
    vmem = pl.BlockSpec(memory_space=pltpu.VMEM)
    hbm = pl.BlockSpec(memory_space=pltpu.HBM)
    dma = pltpu.SemaphoreType.DMA
    wide = 2 * LANES
    one_shape = (SLOTS, NB * AGGS, NB)
    return pl.pallas_call(
        kernel,
        name="galerkin",
        out_shape=(
            jax.ShapeDtypeStruct(one_shape, F32),
            jax.ShapeDtypeStruct((SLOTS * 2 * NB, NB), F32),
        ),
        in_specs=[hbm] * 11,
        out_specs=(vmem, vmem),
        scratch_shapes=[
            pltpu.VMEM((NB, NB, LANES), BF16),
            pltpu.VMEM((NB, NB, LANES), BF16),
            pltpu.VMEM((FACES, LANES), jnp.int32),
            pltpu.VMEM((FACES, LANES), jnp.int32),
            pltpu.VMEM((1, LANES), jnp.int32),
            pltpu.VMEM((PEERS, HALO), jnp.int32),
            pltpu.VMEM((NB * AGGS, NB), F32),
            pltpu.SMEM((SLOTS, AGGS), jnp.int32),
            pltpu.SMEM((SLOTS, AGGS), jnp.int32),
            pltpu.SMEM((1, AGGS), jnp.int32),
            pltpu.VMEM((PAD * PITCH, LANES), F32),
            pltpu.VMEM((ROWS, LANES), BF16),
            pltpu.VMEM((PEERS, QUARTER, LANES), BF16),
            pltpu.VMEM((PEERS, QUARTER, LANES), BF16),
            pltpu.VMEM((PAD * AGGS, PAD), F32),
            pltpu.VMEM((LANES, LANES), F32),
            pltpu.VMEM((LANES, LANES), F32),
            pltpu.VMEM((SUBS - 1, LANES, LANES), F32),
            pltpu.VMEM((FACES, NB, NB, LANES), BF16),
            pltpu.VMEM((FACES + 1, NB, PAD, LANES), F32),
            pltpu.VMEM((ROWS, LANES), F32),
            pltpu.VMEM((ROWS, LANES), F32),
            pltpu.VMEM((FACES + 1, NB // 2, PAD, wide), BF16),
            pltpu.VMEM((FACES * SLOTS, 8, wide), BF16),
            pltpu.VMEM((AGGS, 16, LANES), BF16),
            pltpu.VMEM((AGGS * PAD, NB * LANES), BF16),
            pltpu.VMEM((SLOTS * PAD, NB * LANES), BF16),
            pltpu.VMEM((FACES, 3 * LANES, LANES), BF16),
            pltpu.VMEM((GROUPS, PEERS * LANES, wide), BF16),
            pltpu.VMEM((ROWS, 3 * LANES), BF16),
            pltpu.VMEM((AGGS * PAD, wide), F32),
            pltpu.VMEM((SUBS * AGGS, PAD, wide), BF16),
            pltpu.VMEM((SUBS * AGGS, PAD, wide), BF16),
            pltpu.VMEM((SLOTS, PAD, wide), BF16),
            pltpu.VMEM((AGGS, SLOTS * PAD, wide), BF16),
            pltpu.VMEM((AGGS, SLOTS * PAD, wide), BF16),
            pltpu.VMEM((AGGS * PAD, wide), F32),
            pltpu.VMEM((GROUPS, SLOTS * PAD, LANES), F32),
            pltpu.VMEM((SLOTS * PAD, wide), F32),
            pltpu.VMEM((SLOTS * PAD, wide), BF16),
            pltpu.VMEM((SUBS - 1, 2 * PAD, wide), BF16),
            dma((11,)),
            dma((PEERS,)), dma((PEERS,)),
            dma((SUBS - 1,)), dma((SUBS - 1,)),
            dma((SUBS - 1,)), dma((SUBS - 1,)),
        ],
        compiler_params=pltpu.CompilerParams(
            collective_id=0, has_side_effects=True, vmem_limit_bytes=42 * 2**20
        ),
    )(*[pltpu.with_memory_space_constraint(a, pltpu.HBM) for a in arrays])


def place_kernel(one_ref, two_ref, one_hbm, two_hbm, sem):
    copies = [pltpu.make_async_copy(two_ref, two_hbm, sem.at[SLOTS])]
    for j in range(SLOTS):
        copies.append(pltpu.make_async_copy(one_ref.at[j], one_hbm.at[j], sem.at[j]))
    for copy in copies:
        copy.start()
    for copy in copies:
        copy.wait()


def place_call(one, two):
    anywhere = pl.BlockSpec(memory_space=pl.ANY)
    return pl.pallas_call(
        place_kernel,
        name="place",
        out_shape=(
            jax.ShapeDtypeStruct(one.shape, F32),
            jax.ShapeDtypeStruct(two.shape, F32),
        ),
        in_specs=[anywhere] * 2,
        out_specs=(anywhere,) * 2,
        scratch_shapes=[pltpu.SemaphoreType.DMA((SLOTS + 1,))],
        compiler_params=pltpu.CompilerParams(vmem_limit_bytes=2**20),
    )(one, two)


def per_device(
    diag_block, face_block, restrict1, neighbour, face_slot, agg_map,
    send_list, restrict2, coarse_nbr, agg2_map, coarse_slot,
):
    level = restrict2.transpose(0, 2, 1).reshape(NB * AGGS, NB)
    one, two = fused_call(
        restrict1, diag_block, neighbour, face_slot, agg_map.reshape(1, LANES), send_list, level,
        coarse_nbr, coarse_slot, agg2_map.reshape(1, AGGS), face_block,
    )
    one, two = place_call(one, two)
    one = one.reshape(SLOTS, NB, AGGS, NB).transpose(0, 1, 3, 2)
    two = two.reshape(SLOTS, NB, 2, NB).transpose(0, 1, 3, 2)
    return one, two


def solution(mesh):
    both = ("dom", "sub")
    placed = (
        P(None, None, both), P(None, None, None, both), P(None, None, both),
        P(None, both), P(None, both), P(both), P(None, both),
        P(None, None, both), P(None, both), P(both), P(None, both),
    )
    return jax.shard_map(
        per_device,
        mesh=mesh,
        in_specs=placed,
        out_specs=(P(None, None, None, both), P(None, None, None, both)),
        check_vma=False,
    )
```
